32 devices in a mesh: mer: 8 (over z, x), box: 4 (over y, core).
Axes of the slice: x: 2, y: 2, z: 4, core: 2. Of those that a mesh axis runs over, the one named last changes fastest.
Arguments:
- annulus: float32 [25, 512, 1024], P(None, 'box', 'mer'), may hold values from -6 to 6
- annulus_prev: float32 [25, 512, 1024], P(None, 'box', 'mer'), may hold values from -6 to 6
- derivative: float32 [25, 25], replicated, may hold values from -1.25 to 1.25
- radial_modulus: float32 [25, 1024], P(None, 'mer'), may hold values from 0.5 to 2
- shear_modulus: float32 [25, 1024], P(None, 'mer'), may hold values from 0.5 to 2
- node_mass: float32 [25, 1024], P(None, 'mer'), may hold values from 1 to 4
- element_modes: int32 [1024], P('mer'), may hold values from 1 to 256
- upper_rows: int32 [2048], P('mer'), may hold values from 0 to 3199
- lower_rows: int32 [2048], P('mer'), may hold values from 0 to 3199
- coupling_rows: int32 [16384], P('mer'), may hold values from 0 to 3199
- coupling_target: int32 [16384, 1], P('mer'), may hold values from 0 to 31; in each aligned block of 2048 rows (0 to 2047, 2048 to 4095, ...) at most 128 rows name the same one
- box_field: float32 [32768], P(('mer', 'box')), may hold values from -6 to 6
- box_prev: float32 [32768], P(('mer', 'box')), may hold values from -6 to 6
- box_angle: float32 [32768], P(('mer', 'box')), may hold values from -3.140625 to 3.140625
- box_spring: float32 [32768], P(('mer', 'box')), may hold values from 0.5 to 2
- box_mass: float32 [32768], P(('mer', 'box')), may hold values from 1 to 4
- box_weight: float32 [32768], P(('mer', 'box')), may hold values from 0.05 to 0.5
- box_slot: int32 [32768], P(('mer', 'box')), may hold values from 0 to 1023, as said below
Outputs:
- annulus_out: float32 [25, 512, 1024], P(None, 'box', 'mer')
- box_out: float32 [32768], P(('mer', 'box'))
The draws below stay inside these ranges and needn't reach their ends.
Inputs may be any that keep to these rules, and one draw needn't show every extreme that they name: `lower_rows`: part rows, paired with the previous part's upper rows. `coupling_target`: among the 2048 rows of one part no box part is named more than 128 times, and some box part exactly 128 times. `box_slot`: slot p * 8 + i of the node's box part: the p-th coupling row that part i sends there; slots that no row fills hold zeros. Among the 1024 nodes of one box part, exactly 128 read slots of each meridional part i.
All inputs are finite; a program needn't handle non-finite values.
Results may differ from the reference program's by a relative error of at most 0.0003.
Values sent between devices are 32-bit elements; how exact they have to be, the bound alone decides.
No kernel may reach another device: no remote copies, remote signals or barrier semaphores. Data moves between devices by JAX's collectives and lax.ppermute only.
A program may use at most 128 MiB of HBM per device.

```python
import math
import jax
import jax.numpy as jnp
import numpy as np
from jax import lax

NODES = 25
MODES = 256
E_DEV = 128
SHB = 256
CPL = 2048
BN_DEV = 1024
STEPS = 2
ELEMS = 1024
CAP = 128
SLOTS = 1024
BOXN = 32768
N_MER = 8
DEVICES = 32


def draw_box_slot(key, part):
    first = jax.random.fold_in(key, 11)
    second = jax.random.fold_in(key, 23)
    base = jnp.arange(BN_DEV, dtype=jnp.int32) % N_MER
    source = jax.vmap(lambda single: jax.random.permutation(single, base))(jax.random.split(first, DEVICES))
    places = jax.random.randint(second, (DEVICES, BN_DEV), 0, CAP, dtype=jnp.int32)
    return (places * N_MER + source).reshape(-1).astype(jnp.int32)


def touch_ends(array, key, least, top_value):
    dims = array.shape
    spot = [jax.random.randint(jax.random.fold_in(key, axis), (), 0, dims[axis]) for axis in range(len(dims))]
    array = array.at[tuple(spot)].set(least)
    longest = dims.index(max(dims))
    spot[longest] = (spot[longest] + 1) % dims[longest]
    return array.at[tuple(spot)].set(top_value)


def block_levels(own_key, dims, pieces, least, high):
    gain = 1.0
    for dim, blocks in pieces:
        steps = jax.random.uniform(jax.random.fold_in(jax.random.fold_in(own_key, 6), dim), (blocks,), jnp.float32, least / len(pieces), high / len(pieces))
        gain = gain * jnp.repeat(jnp.exp(steps), dims[dim] // blocks).reshape((-1,) + (1,) * (len(dims) - 1 - dim))
    return gain


def shared_out(own_key, own, number, rows, count, top, bound, lean):
    ranking = jax.random.permutation(own_key, count)
    heavy_load, common = portions_of(count, rows * top, bound, lean, True), portions_of(count, rows * top, bound, lean, False)
    places = jnp.arange(count)

    def named(lengths, turn):
        used = int((lengths > 0).sum())
        fixed = max(1, used // 4)
        shifted = fixed + (places - fixed + turn * (used - fixed)) % max(1, count - fixed)
        return jnp.zeros((count,), jnp.int32).at[ranking[jnp.where(places < fixed, places, shifted)]].set(jnp.asarray(lengths, jnp.int32))

    lengths = jnp.where(number % 4 == 0, named(heavy_load, number // 4), named(common, number - number // 4 - 1))
    mixed = jax.random.permutation(jax.random.fold_in(own, 3), count)
    giver, receiver = mixed[0:count // 2 * 2:2], mixed[1:count // 2 * 2:2]
    room = jnp.minimum(lengths[giver] - 1, bound - lengths[receiver]) // 2
    room = jnp.where((giver == ranking[0]) | (receiver == ranking[0]) | (lengths[receiver] == 0), 0, jnp.maximum(room, 0))
    shifted = jax.random.randint(jax.random.fold_in(own, 4), (count // 2,), 0, 1 << 20) % (room + 1)
    lengths = lengths.at[giver].add(-shifted).at[receiver].add(shifted)
    labels = jnp.searchsorted(jnp.cumsum(lengths), jnp.arange(rows * top), side="right").astype(jnp.int32)
    table = labels.reshape(top, rows).T
    table = table[jax.random.permutation(jax.random.fold_in(own, 1), rows)]
    turn = jax.random.randint(jax.random.fold_in(own, 2), (rows, 1), 0, top)
    return jnp.take_along_axis(table, (jnp.arange(top)[None, :] + turn) % top, axis=1)


def portions_of(amount, total, limit, lean, full):
    weights = [(1 << 20) // math.isqrt(grade ** lean) + 1 for grade in range(1, amount + 1)]
    largest = limit if full else min(limit, max(-(-total // amount), total * weights[0] // sum(weights)))
    least = 1 if total - largest >= amount - 1 else 0
    given, spare = [largest] + [least] * (amount - 1), total - largest - least * (amount - 1)
    while spare > 0:
        movable = [i for i in range(1, amount) if given[i] < largest] or [i for i in range(1, amount) if given[i] < limit]
        mass, left = sum([weights[i] for i in movable]), spare
        for i in movable:
            extra = min(limit - given[i], max(1, left * weights[i] // mass), spare)
            given[i] = given[i] + extra
            spare = spare - extra
    return np.array(given)


def gaussian(rng, dims, width, most, cuts=(), kind=jnp.bfloat16):
    entries = jax.random.normal(rng, dims, jnp.float32) * width
    if len(cuts) > 0:
        entries = block_levels(rng, dims, cuts, -0.22, 0.18) * entries
    return jnp.clip(entries, min=-most, max=most).astype(kind)


def setup_inputs(seed: int = 0) -> dict:
    keys = jax.random.split(jax.random.key(seed), 19)
    annulus = gaussian(keys[0], (NODES, 2 * MODES, ELEMS), 1.0, 6.0, ((1, 4), (2, 8)), jnp.float32)
    annulus_prev = gaussian(keys[1], (NODES, 2 * MODES, ELEMS), 1.0, 6.0, ((1, 4), (2, 8)), jnp.float32)
    derivative = gaussian(keys[2], (NODES, NODES), NODES ** -0.5, 1.25, (), jnp.float32)
    radial_modulus = jnp.clip(jnp.exp(math.log(2.0) - 1.3862944 * jax.random.uniform(keys[3], (NODES, ELEMS), jnp.float32) ** block_levels(keys[3], (NODES, ELEMS), ((1, 8),), -0.2, 0.2)), 0.5, 2.0)
    shear_modulus = jnp.clip(jnp.exp(math.log(2.0) - 1.3862944 * jax.random.uniform(keys[4], (NODES, ELEMS), jnp.float32) ** block_levels(keys[4], (NODES, ELEMS), ((1, 8),), -0.2, 0.2)), 0.5, 2.0)
    node_mass = jnp.clip(jnp.exp(math.log(4.0) - 1.3862944 * jax.random.uniform(keys[5], (NODES, ELEMS), jnp.float32) ** block_levels(keys[5], (NODES, ELEMS), ((1, 8),), -0.2, 0.2)), 1.0, 4.0)
    element_modes = touch_ends(jax.random.randint(keys[6], (ELEMS,), 1, MODES + 1), jax.random.fold_in(keys[6], 1), 1, MODES).astype(jnp.int32)
    upper_rows = touch_ends(jax.random.randint(keys[7], (N_MER * SHB,), 0, NODES * E_DEV), jax.random.fold_in(keys[7], 1), 0, (NODES * E_DEV) - 1).astype(jnp.int32)
    lower_rows = touch_ends(jax.random.randint(keys[8], (N_MER * SHB,), 0, NODES * E_DEV), jax.random.fold_in(keys[8], 1), 0, (NODES * E_DEV) - 1).astype(jnp.int32)
    coupling_rows = touch_ends(jax.random.randint(keys[9], (N_MER * CPL,), 0, NODES * E_DEV), jax.random.fold_in(keys[9], 1), 0, (NODES * E_DEV) - 1).astype(jnp.int32)
    coupling_target_keys = jax.random.split(jax.random.fold_in(keys[10], 1), (N_MER * CPL) // CPL)
    coupling_target_turns = jax.random.permutation(jax.random.fold_in(keys[10], 3), (N_MER * CPL) // CPL)
    coupling_target = jax.vmap(lambda own, number: shared_out(jax.random.fold_in(keys[10], 2), own, number, CPL, DEVICES, 1, CAP, 2))(coupling_target_keys, coupling_target_turns).reshape((N_MER * CPL, 1))
    box_field = gaussian(keys[11], (BOXN,), 1.0, 6.0, ((0, 32),), jnp.float32)
    box_prev = gaussian(keys[12], (BOXN,), 1.0, 6.0, ((0, 32),), jnp.float32)
    box_angle = jnp.clip(jax.random.uniform(keys[13], (BOXN,), jnp.float32, -3.140625, 3.140625), -3.140625, 3.140625)
    box_spring = jnp.clip(jnp.exp(math.log(2.0) - 1.3862944 * jax.random.uniform(keys[14], (BOXN,), jnp.float32) ** block_levels(keys[14], (BOXN,), ((0, 32),), -0.2, 0.2)), 0.5, 2.0)
    box_mass = jnp.clip(jnp.exp(math.log(4.0) - 1.3862944 * jax.random.uniform(keys[15], (BOXN,), jnp.float32) ** block_levels(keys[15], (BOXN,), ((0, 32),), -0.2, 0.2)), 1.0, 4.0)
    box_weight = jnp.clip(jnp.exp(math.log(0.5) - 2.3025851 * jax.random.uniform(keys[16], (BOXN,), jnp.float32) ** block_levels(keys[16], (BOXN,), ((0, 32),), -0.2, 0.2)), 0.05, 0.5)
    box_slot = draw_box_slot(jax.random.fold_in(keys[18], 71), 0)
    return dict(annulus=annulus, annulus_prev=annulus_prev, derivative=derivative, radial_modulus=radial_modulus, shear_modulus=shear_modulus, node_mass=node_mass, element_modes=element_modes, upper_rows=upper_rows, lower_rows=lower_rows, coupling_rows=coupling_rows, coupling_target=coupling_target, box_field=box_field, box_prev=box_prev, box_angle=box_angle, box_spring=box_spring, box_mass=box_mass, box_weight=box_weight, box_slot=box_slot)


step_scale = 0.25


def azimuth_basis(angles):
    column = jnp.arange(2 * MODES, dtype=jnp.int32)
    order = (column % MODES).astype(jnp.float32)
    phase = angles[:, None] * order[None, :]
    return jnp.where(column[None, :] < MODES, jnp.cos(phase), jnp.sin(phase))


def annulus_force(values, derivative, radial_modulus, shear_modulus, wavenum):
    node_count, column_count, element_count = values.shape
    flat = values.reshape(node_count, column_count * element_count)
    gradient = jnp.dot(derivative, flat, precision=lax.Precision.HIGHEST)
    gradient = gradient.reshape(node_count, column_count, element_count)
    flux = (radial_modulus[:, None, :] * gradient).reshape(node_count, column_count * element_count)
    backward = jnp.dot(derivative.T, flux, precision=lax.Precision.HIGHEST)
    backward = backward.reshape(node_count, column_count, element_count)
    return -backward - shear_modulus[:, None, :] * wavenum[None, :, None] * values


def box_part(packed):
    coefficients, slot_ids, angles, springs, weights, positions = packed
    harmonic = azimuth_basis(angles)
    sample = jnp.sum(coefficients[slot_ids] * harmonic, axis=1)
    pull = springs * (sample - positions)
    reaction = jax.ops.segment_sum((-weights * pull)[:, None] * harmonic, slot_ids, num_segments=SLOTS)
    return pull, reaction


def reference(annulus, annulus_prev, derivative, radial_modulus, shear_modulus, node_mass, element_modes, upper_rows, lower_rows, coupling_rows, coupling_target, box_field, box_prev, box_angle, box_spring, box_mass, box_weight, box_slot):
    column = jnp.arange(2 * MODES, dtype=jnp.int32)
    order = (column % MODES).astype(jnp.float32)
    wavenum = (2.0 * order / MODES) ** 2
    live_mask = ((column % MODES)[:, None] < element_modes[None, :]).astype(jnp.float32)
    part_index = jnp.arange(N_MER, dtype=jnp.int32)[:, None]
    upper_part = upper_rows.reshape(N_MER, SHB)
    lower_part = lower_rows.reshape(N_MER, SHB)
    upper_node = upper_part // E_DEV
    upper_element = part_index * E_DEV + upper_part % E_DEV
    lower_node = lower_part // E_DEV
    lower_element = part_index * E_DEV + lower_part % E_DEV
    coupled = coupling_rows.reshape(N_MER, CPL)
    coupled_node = coupled // E_DEV
    coupled_element = part_index * E_DEV + coupled % E_DEV
    target = coupling_target[:, 0].reshape(N_MER, CPL)
    target_hot = (target[:, :, None] == jnp.arange(DEVICES, dtype=jnp.int32)[None, None, :]).astype(jnp.int32)
    position = jnp.sum((jnp.cumsum(target_hot, axis=1) - target_hot) * target_hot, axis=2)
    global_slot = (target * SLOTS + position * N_MER + part_index).reshape(-1).astype(jnp.int32)
    slot_parts = box_slot.reshape(DEVICES, BN_DEV)
    angle_parts = box_angle.reshape(DEVICES, BN_DEV)
    spring_parts = box_spring.reshape(DEVICES, BN_DEV)
    weight_parts = box_weight.reshape(DEVICES, BN_DEV)
    current = annulus
    previous = annulus_prev
    box_now = box_field
    box_before = box_prev
    for step_index in range(STEPS):
        force = annulus_force(current, derivative, radial_modulus, shear_modulus, wavenum)
        lower_values = force[lower_node, :, lower_element]
        upper_values = force[upper_node, :, upper_element]
        empty_rows = jnp.zeros((1, SHB, 2 * MODES), jnp.float32)
        from_below = jnp.concatenate([empty_rows, upper_values[:-1]], axis=0)
        from_above = jnp.concatenate([lower_values[1:], empty_rows], axis=0)
        force = force.at[lower_node, :, lower_element].add(from_below)
        force = force.at[upper_node, :, upper_element].add(from_above)
        sent_rows = current[coupled_node, :, coupled_element].reshape(N_MER * CPL, 2 * MODES)
        table = jnp.zeros((DEVICES * SLOTS, 2 * MODES), jnp.float32).at[global_slot].set(sent_rows)
        table = table.reshape(DEVICES, SLOTS, 2 * MODES)
        pull, reaction = lax.map(box_part, (table, slot_parts, angle_parts, spring_parts, weight_parts, box_now.reshape(DEVICES, BN_DEV)))
        returned = reaction.reshape(DEVICES * SLOTS, 2 * MODES)[global_slot].reshape(N_MER, CPL, 2 * MODES)
        force = force.at[coupled_node, :, coupled_element].add(returned)
        annulus_next = 2.0 * current - previous + step_scale * live_mask[None, :, :] * force / node_mass[:, None, :]
        box_next = 2.0 * box_now - box_before + step_scale * pull.reshape(-1) / box_mass
        previous = current
        current = annulus_next
        box_before = box_now
        box_now = box_next
    return current, box_now
```

```python
import functools

import jax
import jax.numpy as jnp
from jax import lax
from jax.experimental import pallas as pl
from jax.experimental.pallas import tpu as pltpu
from jax.sharding import PartitionSpec as P

MODES = 256
STEPS = 2
LANES = 128
WIDE = 256

step_scale = 0.25
f32 = jnp.float32
bf16 = jnp.bfloat16
i32 = jnp.int32


def iota(shape, dim):
    return lax.broadcasted_iota(i32, shape, dim)


def dot(a, b):
    return lax.dot_general(a, b, (((1,), (0,)), ((), ())), preferred_element_type=f32)


def dot_nt(a, b):
    return lax.dot_general(a, b, (((1,), (1,)), ((), ())), preferred_element_type=f32)


def hot(mask):
    return jnp.where(mask, 1.0, 0.0).astype(bf16)


def split(x):
    high = x.astype(bf16)
    return high, (x - high.astype(f32)).astype(bf16)


def stacked(x):
    high, low = split(x)
    return jnp.concatenate([high, low], axis=0)


def folded(x):
    half = x.shape[0] // 2
    return x[:half] + x[half:]


def running(mask):
    rows, width = mask.shape
    below = hot(iota((LANES, LANES), 0) < iota((LANES, LANES), 1))
    total = jnp.zeros((rows, 1), f32)
    counts = []
    for start in range(0, width, LANES):
        block = mask[:, start : start + LANES]
        counts.append(dot(block.astype(bf16), below) + total)
        total = total + jnp.sum(block, axis=1, keepdims=True)
    return jnp.concatenate(counts, axis=1), total


def group_kernel(parts, copies, slot_ref, *refs):
    fields, (out_ref, dest_ref, stack_ref) = refs[:6], refs[6:]
    nodes = slot_ref.shape[1]
    per = nodes // parts
    slot = slot_ref[...].astype(f32)
    place = jnp.floor((slot + 0.5) * (1.0 / parts))
    part = slot - place * parts
    rows = max(16, parts)
    mask = jnp.where(iota((rows, nodes), 0) == part.astype(i32), 1.0, 0.0)
    count, _ = running(mask)
    dest = (part * per + jnp.sum(mask * count, axis=0, keepdims=True)).astype(i32)
    dest_ref[...] = dest
    stack_ref[...] = jnp.zeros_like(stack_ref)
    stack_ref[0:1, :] = place
    for index, field in enumerate(fields):
        stack_ref[index + 1 : index + 2, :] = field[...]
    values = stack_ref[...]
    first = values.astype(bf16).astype(f32)
    second = (values - first).astype(bf16).astype(f32)
    third = values - first - second
    terms = jnp.concatenate([first, second, third, jnp.zeros_like(third)], axis=0).astype(bf16)
    for start in range(0, nodes, WIDE):
        moved = dot_nt(terms, hot(iota((WIDE, nodes), 0) + start == dest))
        moved = moved[0:8] + moved[8:16] + moved[16:24]
        for lane in range(0, WIDE, per):
            for copy in range(copies):
                out_ref[(start + lane) // per * copies + copy] = moved[:, lane : lane + per]


def ungroup_kernel(dest_ref, value_ref, out_ref):
    nodes = dest_ref.shape[1]
    values = value_ref[...]
    first = values.astype(bf16).astype(f32)
    second = (values - first).astype(bf16).astype(f32)
    third = values - first - second
    terms = jnp.concatenate(
        [first, second, third, jnp.zeros((13, nodes), f32)], axis=0
    ).astype(bf16)
    dest = dest_ref[...]
    for start in range(0, nodes, WIDE):
        back = dot(terms, hot(iota((nodes, WIDE), 0) == dest[:, start : start + WIDE]))
        out_ref[:, start : start + WIDE] = back[0:1] + back[1:2] + back[2:3]


def rows_kernel(
    elements, target_ref, rows_ref, lower_ref, upper_ref, key_ref, keycol_ref, off_ref, cnt_ref, win_ref
):
    blocks = off_ref.shape[0]
    count = target_ref.shape[1]
    shared = lower_ref.shape[1]
    mask = jnp.where(iota((blocks, count), 0) == target_ref[...], 1.0, 0.0)
    before, total = running(mask)
    totals = jnp.broadcast_to(total, (blocks, LANES))
    offset = dot(hot(iota((blocks, blocks), 1) < iota((blocks, blocks), 0)), totals.astype(bf16))
    off_ref[...] = offset
    cnt_ref[...] = totals
    window = jnp.floor(offset * (1.0 / LANES)) * LANES
    win_ref[...] = jnp.minimum(window, count - WIDE).astype(i32)
    place = jnp.sum(mask * (before + offset[:, 0:1]), axis=0, keepdims=True).astype(i32)
    row = rows_ref[...].astype(f32)
    node = jnp.floor((row + 0.5) * (1.0 / elements))
    terms = jnp.concatenate(
        [node, row - node * elements, jnp.zeros((14, count), f32)], axis=0
    ).astype(bf16)
    for start in range(0, count, WIDE):
        moved = dot_nt(terms, hot(iota((WIDE, count), 0) + start == place))
        key_ref[:, start : start + WIDE] = (moved[0:1] * elements + moved[1:2]).astype(i32)
    key_ref[:, count : count + shared] = lower_ref[...]
    key_ref[:, count + shared : count + 2 * shared] = upper_ref[...]
    for start in range(0, count + 2 * shared, LANES):
        block = jnp.broadcast_to(key_ref[:, start : start + LANES].astype(f32), (LANES, LANES))
        keycol_ref[start : start + LANES, :] = block.T.astype(i32)


def fill_stack(value_ref, stack_ref):
    nodes, columns, elements = value_ref.shape
    for node in range(nodes):
        high, low = split(value_ref[node])
        lanes = slice(node * elements, (node + 1) * elements)
        stack_ref[0:columns, lanes] = high
        stack_ref[columns:, lanes] = low
    if stack_ref.shape[1] > nodes * elements:
        tail = slice(nodes * elements, stack_ref.shape[1])
        stack_ref[:, tail] = jnp.zeros_like(stack_ref[:, tail])


def picked(stack_ref, hot_ref, key_ref, start):
    depth = stack_ref.shape[1]
    key = key_ref[:, pl.ds(start, WIDE)]
    base = iota((LANES, WIDE), 0)
    for row in range(0, depth, LANES):
        hot_ref[row : row + LANES, :] = hot(base == key - row)
    return dot(stack_ref[...], hot_ref[0:depth, :])


def pick_rows(stack_ref, hot_ref, key_ref, out_ref):
    def body(index, carry):
        start = pl.multiple_of(index * WIDE, WIDE)
        out_ref[:, pl.ds(start, WIDE)] = picked(stack_ref, hot_ref, key_ref, start).astype(bf16)
        return carry

    lax.fori_loop(0, out_ref.shape[1] // WIDE, body, 0)


def pick_boundary(stack_ref, hot_ref, key_ref, low_ref, high_ref):
    shared = low_ref.shape[1]
    first = key_ref.shape[1] - 2 * shared
    for ref, origin in ((low_ref, first), (high_ref, first + shared)):
        for start in range(0, shared, WIDE):
            ref[:, start : start + WIDE] = folded(
                picked(stack_ref, hot_ref, key_ref, origin + start)
            )


def spread(derivative_ref, transposed, rows):
    nodes = derivative_ref.shape[0]
    size = 8 * nodes
    left = jnp.where(iota((rows, nodes), 0) // 8 == iota((rows, nodes), 1), 1.0, 0.0)
    right = jnp.where(iota((nodes, size), 1) // 8 == iota((nodes, size), 0), 1.0, 0.0)
    dims = (((1,), (1,)), ((), ())) if transposed else (((1,), (0,)), ((), ()))
    half = lax.dot_general(
        left, derivative_ref[...], dims, precision=lax.Precision.HIGHEST, preferred_element_type=f32
    )
    full = jnp.dot(half, right, precision=lax.Precision.HIGHEST, preferred_element_type=f32)
    full = jnp.where(iota((rows, size), 0) % 8 == iota((rows, size), 1) % 8, full, 0.0)
    return stacked(full)


def force_into(value_ref, derivative_ref, radial_ref, shear_ref, first_order, force_ref):
    nodes, columns, elements = value_ref.shape
    size = 8 * nodes
    rows = -(-size // 16) * 16
    forward = spread(derivative_ref, False, rows)
    backward = spread(derivative_ref, True, rows)
    radial = jnp.broadcast_to(radial_ref[...][:, None, :], (nodes, 8, elements)).reshape(
        size, elements
    )
    radial = jnp.concatenate([radial, radial], axis=1)
    shear = jnp.broadcast_to(shear_ref[...][:, None, :], (nodes, 8, elements))

    def applied(matrix, x):
        high, low = split(x)
        both = dot(matrix, high)
        return both[:size] + both[rows : rows + size] + dot(matrix[:rows], low)[:size]

    def body(index, carry):
        start = pl.multiple_of(index * 16, 16)
        halves = [value_ref[:, pl.ds(start, 8), :], value_ref[:, pl.ds(start + 8, 8), :]]
        x = jnp.concatenate([half.reshape(size, elements) for half in halves], axis=1)
        back = applied(backward, radial * applied(forward, x))
        for side, half in enumerate(halves):
            order = (first_order + start + 8 * side + iota((8, elements), 0)).astype(f32)
            wave = (2.0 * order / MODES) ** 2
            block = back[:, side * elements : (side + 1) * elements].reshape(nodes, 8, elements)
            force_ref[:, pl.ds(start + 8 * side, 8), :] = -block - shear * wave[None] * half
        return carry

    lax.fori_loop(0, columns // 16, body, 0)


def start_kernel(
    box_ref, value_ref, derivative_ref, radial_ref, shear_ref, key_ref,
    force_ref, low_ref, high_ref, picked_ref, stack_ref, hot_ref,
):
    columns = value_ref.shape[1]
    force_into(
        value_ref, derivative_ref, radial_ref, shear_ref, box_ref[0] * columns % MODES, force_ref
    )
    fill_stack(force_ref, stack_ref)
    pick_boundary(stack_ref, hot_ref, key_ref, low_ref, high_ref)
    fill_stack(value_ref, stack_ref)
    pick_rows(stack_ref, hot_ref, key_ref, picked_ref)


def window_hot(win_ref, place_ref, group, stride):
    window = pl.multiple_of(win_ref[group * stride, 0], LANES)
    place = place_ref[pl.ds(group, 1), :]
    return window, hot(iota((WIDE, LANES), 0) + window == place)


def sample_into(win_ref, place_ref, harmonic_ref, picked_ref, stride, sample_ref):
    def body(group, carry):
        window, chosen = window_hot(win_ref, place_ref, group, stride)
        rows = folded(dot(picked_ref[:, pl.ds(window, WIDE)], chosen))
        sample_ref[pl.ds(group, 1), :] = jnp.sum(
            rows * harmonic_ref[group], axis=0, keepdims=True
        )
        return carry

    lax.fori_loop(0, sample_ref.shape[0], body, 0)


def node_kernel(
    stride, box_ref, win_ref, message_ref, off_ref, cnt_ref, picked_ref,
    harmonic_ref, place_ref, node_ref, sample_ref,
    near_re, near_im, far_re, far_im,
):
    groups, columns, _ = harmonic_ref.shape
    place = message_ref[:, 0, :]
    angle = message_ref[:, 1, :]
    place_ref[...] = jnp.where(place < cnt_ref[...], off_ref[...] + place, -1.0).astype(i32)
    for index in range(5):
        node_ref[index] = message_ref[:, 2 + index, :]

    def power(order):
        return jnp.cos(order * angle), jnp.sin(order * angle)

    def times(x, y):
        return x[0] * y[0] - x[1] * y[1], x[0] * y[1] + x[1] * y[0]

    near = [(jnp.ones_like(angle), jnp.zeros_like(angle))] + [None] * 7
    for bit in (1, 2, 4):
        factor = power(float(bit))
        near[bit] = factor
        for low in range(1, bit):
            near[bit + low] = times(factor, near[low])
    for index, (re, im) in enumerate(near):
        near_re[:, index, :] = re
        near_im[:, index, :] = im
    first = box_ref[0] * columns
    base_re, base_im = power((first % MODES).astype(f32))
    sine = first >= MODES
    far = [
        (jnp.where(sine, base_im, base_re), jnp.where(sine, -base_re, base_im))
    ] + [None] * (columns // 8 - 1)
    bit = 1
    while bit < columns // 8:
        factor = power(float(8 * bit))
        for low in range(min(bit, columns // 8 - bit)):
            far[bit + low] = times(factor, far[low])
        bit *= 2
    for index, (re, im) in enumerate(far):
        far_re[index] = re
        far_im[index] = im

    def body(group, carry):
        re, im = near_re[group], near_im[group]
        for index in range(columns // 8):
            harmonic_ref[group, 8 * index : 8 * index + 8, :] = (
                far_re[index, pl.ds(group, 1), :] * re - far_im[index, pl.ds(group, 1), :] * im
            )
        return carry

    lax.fori_loop(0, groups, body, 0)
    sample_into(win_ref, place_ref, harmonic_ref, picked_ref, stride, sample_ref)


def nodes_step(samples_ref, node_ref, now, before, next_ref, coefficient_ref):
    sample = samples_ref[0]
    for index in range(1, samples_ref.shape[0]):
        sample = sample + samples_ref[index]
    pull = node_ref[0] * (sample - now)
    next_ref[...] = 2.0 * now - before + step_scale * pull / node_ref[1]
    coefficient_ref[...] = -node_ref[2] * pull


def annulus_step(
    stride, first_order, win_ref, place_ref, harmonic_ref, coefficient_ref, keycol_ref,
    below_ref, above_ref, value_ref, previous_ref, force_ref, mass_ref, modes_ref,
    next_ref, reaction_ref, terms_ref, hot_ref, added_ref,
):
    nodes, columns, elements = value_ref.shape
    groups = place_ref.shape[0]
    count = reaction_ref.shape[1]
    shared = below_ref.shape[1]
    reaction_ref[...] = jnp.zeros_like(reaction_ref)

    def react(group, carry):
        window, chosen = window_hot(win_ref, place_ref, group, stride)
        weighted = harmonic_ref[group] * coefficient_ref[pl.ds(group, 1), :]
        rows = folded(dot_nt(stacked(weighted), chosen))
        reaction_ref[:, pl.ds(window, WIDE)] = reaction_ref[:, pl.ds(window, WIDE)] + rows
        return carry

    lax.fori_loop(0, groups, react, 0)
    terms_ref[:, 0:count] = stacked(reaction_ref[...])
    terms_ref[:, count : count + shared] = stacked(below_ref[...])
    terms_ref[:, count + shared : count + 2 * shared] = stacked(above_ref[...])
    depth = count + 2 * shared
    lane = iota((LANES, LANES), 1)

    def place_rows(pair, carry):
        for side in range(2):
            base = lane + (2 * pair + side) * elements
            for row in range(0, depth, LANES):
                hot_ref[row : row + LANES, side * LANES : (side + 1) * LANES] = hot(
                    keycol_ref[row : row + LANES, :] == base
                )
        rows = folded(dot(terms_ref[...], hot_ref[0:depth, :]))
        added_ref[2 * pair] = rows[:, 0:LANES]
        added_ref[2 * pair + 1] = rows[:, LANES:]
        return carry

    lax.fori_loop(0, added_ref.shape[0] // 2, place_rows, 0)
    order = first_order + iota((columns, elements), 0)
    live = jnp.where(order < modes_ref[...], step_scale, 0.0)
    for node in range(nodes):
        gain = live / mass_ref[node : node + 1, :]
        next_ref[node] = (
            2.0 * value_ref[node]
            - previous_ref[node]
            + gain * (force_ref[node] + added_ref[node])
        )


def middle_kernel(
    stride, box_ref, win_ref, samples_ref, node_ref, place_ref, harmonic_ref, keycol_ref, key_ref,
    below_ref, above_ref, value_ref, previous_ref, force_ref, mass_ref, modes_ref,
    derivative_ref, radial_ref, shear_ref,
    next_ref, nextforce_ref, low_ref, high_ref, sample_ref, boxnext_ref,
    coefficient_ref, reaction_ref, terms_ref, hot_ref, added_ref, stack_ref, picked_ref,
):
    columns = value_ref.shape[1]
    first_order = box_ref[0] * columns % MODES
    nodes_step(samples_ref, node_ref, node_ref[3], node_ref[4], boxnext_ref, coefficient_ref)
    annulus_step(
        stride, first_order, win_ref, place_ref, harmonic_ref, coefficient_ref, keycol_ref,
        below_ref, above_ref, value_ref, previous_ref, force_ref, mass_ref, modes_ref,
        next_ref, reaction_ref, terms_ref, hot_ref, added_ref,
    )
    force_into(next_ref, derivative_ref, radial_ref, shear_ref, first_order, nextforce_ref)
    fill_stack(nextforce_ref, stack_ref)
    pick_boundary(stack_ref, hot_ref, key_ref, low_ref, high_ref)
    fill_stack(next_ref, stack_ref)
    pick_rows(stack_ref, hot_ref, key_ref, picked_ref)
    sample_into(win_ref, place_ref, harmonic_ref, picked_ref, stride, sample_ref)


def box_kernel(samples_ref, node_ref, now_ref, boxnext_ref, coefficient_ref):
    nodes_step(samples_ref, node_ref, now_ref[...], node_ref[3], boxnext_ref, coefficient_ref)


def last_kernel(
    stride, box_ref, win_ref, coefficient_ref, place_ref, harmonic_ref, keycol_ref,
    below_ref, above_ref, value_ref, previous_ref, force_ref, mass_ref, modes_ref,
    next_ref, reaction_ref, terms_ref, hot_ref, added_ref,
):
    first_order = box_ref[0] * value_ref.shape[1] % MODES
    annulus_step(
        stride, first_order, win_ref, place_ref, harmonic_ref, coefficient_ref, keycol_ref,
        below_ref, above_ref, value_ref, previous_ref, force_ref, mass_ref, modes_ref,
        next_ref, reaction_ref, terms_ref, hot_ref, added_ref,
    )


def call(kernel, ins, outs, scratch=(), scalars=0, name=None):
    smem = pl.BlockSpec(memory_space=pltpu.SMEM)
    vmem = pl.BlockSpec(memory_space=pltpu.VMEM)
    return pl.pallas_call(
        kernel,
        out_shape=[jax.ShapeDtypeStruct(shape, dtype) for shape, dtype in outs],
        in_specs=[smem] * scalars + [vmem] * (len(ins) - scalars),
        out_specs=[vmem] * len(outs),
        scratch_shapes=[pltpu.VMEM(shape, dtype) for shape, dtype in scratch],
        name=name,
    )(*ins)


def exchanged(low, high):
    size = lax.axis_size("mer")
    up = [(i, i + 1) for i in range(size - 1)]
    down = [(j, i) for i, j in up]
    return lax.ppermute(high, "mer", up), lax.ppermute(low, "mer", down)


def per_device(
    annulus,
    annulus_prev,
    derivative,
    radial_modulus,
    shear_modulus,
    node_mass,
    element_modes,
    upper_rows,
    lower_rows,
    coupling_rows,
    coupling_target,
    box_field,
    box_prev,
    box_angle,
    box_spring,
    box_mass,
    box_weight,
    box_slot,
):
    mer_count = lax.axis_size("mer")
    box_count = lax.axis_size("box")
    blocks = mer_count * box_count
    nodes, columns, elements = annulus.shape
    box_nodes = box_slot.shape[0]
    per = box_nodes // mer_count
    stride = LANES // per
    groups = blocks * per // LANES
    count = coupling_rows.shape[0]
    shared = upper_rows.shape[0]
    depth = count + 2 * shared
    padded_nodes = nodes + nodes % 2
    field = ((nodes, columns, elements), f32)
    side = ((columns, shared), f32)
    grid = ((groups, LANES), f32)
    hot_scratch = ((max(padded_nodes * elements, depth), WIDE), bf16)
    stack_scratch = ((2 * columns, padded_nodes * elements), bf16)
    picked_shape = ((2 * columns, count), bf16)
    box = jnp.full((1,), lax.axis_index("box"), i32)
    modes = element_modes.reshape(1, elements)

    sent = [
        value.reshape(1, box_nodes)
        for value in (box_slot, box_angle, box_spring, box_mass, box_weight, box_field, box_prev)
    ]
    messages, dest = call(
        functools.partial(group_kernel, mer_count, box_count),
        sent,
        [((blocks, 8, per), f32), ((1, box_nodes), i32)],
        [((8, box_nodes), f32)],
        name="group",
    )
    messages = lax.all_to_all(messages, ("mer", "box"), split_axis=0, concat_axis=0, tiled=True)
    if stride > 1:
        messages = messages.reshape(groups, stride, 8, per).swapaxes(1, 2)
        messages = messages.reshape(groups, 8, LANES)

    key, keycol, offset, filled, window = call(
        functools.partial(rows_kernel, elements),
        [
            coupling_target.reshape(1, count),
            coupling_rows.reshape(1, count),
            lower_rows.reshape(1, shared),
            upper_rows.reshape(1, shared),
        ],
        [
            ((1, depth), i32),
            ((depth, LANES), i32),
            ((blocks, LANES), f32),
            ((blocks, LANES), f32),
            ((blocks, LANES), i32),
        ],
        name="rows",
    )
    if stride > 1:
        offset = jnp.repeat(offset[:, 0], per).reshape(groups, LANES)
        filled = jnp.repeat(filled[:, 0], per).reshape(groups, LANES)

    force, low, high, chosen = call(
        start_kernel,
        [box, annulus, derivative, radial_modulus, shear_modulus, key],
        [field, side, side, picked_shape],
        [stack_scratch, hot_scratch],
        scalars=1,
        name="start",
    )
    below, above = exchanged(low, high)

    harmonic, place, node, sample = call(
        functools.partial(node_kernel, stride),
        [box, window, messages, offset, filled, chosen],
        [((groups, columns, LANES), f32), ((groups, LANES), i32), ((5, groups, LANES), f32), grid],
        [((groups, 8, LANES), f32)] * 2 + [((columns // 8, groups, LANES), f32)] * 2,
        scalars=2,
        name="nodes",
    )
    samples = lax.all_gather(sample, "box")

    step_scratch = [
        ((columns, count), f32),
        ((2 * columns, depth), bf16),
        hot_scratch,
        ((padded_nodes, columns, elements), f32),
    ]
    current, force, low, high, sample, box_now = call(
        functools.partial(middle_kernel, stride),
        [
            box, window, samples, node, place, harmonic, keycol, key, below, above, annulus,
            annulus_prev, force, node_mass, modes, derivative, radial_modulus, shear_modulus,
        ],
        [field, field, side, side, grid, grid],
        [grid] + step_scratch + [stack_scratch, picked_shape],
        scalars=2,
        name="middle",
    )
    below, above = exchanged(low, high)
    samples = lax.all_gather(sample, "box")

    box_now, coefficient = call(box_kernel, [samples, node, box_now], [grid, grid], name="box")
    returned = lax.all_to_all(
        box_now.reshape(mer_count, box_count, per), "mer", split_axis=0, concat_axis=0, tiled=True
    )
    returned = lax.dynamic_index_in_dim(
        returned, lax.axis_index("box"), axis=1, keepdims=False
    )
    (box_out,) = call(
        ungroup_kernel, [dest, returned.reshape(1, box_nodes)], [((1, box_nodes), f32)], name="ungroup"
    )
    (current,) = call(
        functools.partial(last_kernel, stride),
        [
            box, window, coefficient, place, harmonic, keycol, below, above, current, annulus,
            force, node_mass, modes,
        ],
        [field],
        step_scratch,
        scalars=2,
        name="last",
    )
    return current, box_out.reshape(box_nodes)


def solution(mesh):
    in_specs = (
        P(None, "box", "mer"),
        P(None, "box", "mer"),
        P(),
        P(None, "mer"),
        P(None, "mer"),
        P(None, "mer"),
        P("mer"),
        P("mer"),
        P("mer"),
        P("mer"),
        P("mer", None),
        P(("mer", "box")),
        P(("mer", "box")),
        P(("mer", "box")),
        P(("mer", "box")),
        P(("mer", "box")),
        P(("mer", "box")),
        P(("mer", "box")),
    )
    out_specs = (P(None, "box", "mer"), P(("mer", "box")))
    return jax.shard_map(
        per_device, mesh=mesh, in_specs=in_specs, out_specs=out_specs, check_vma=False
    )
```

```python
import functools

import jax
import jax.numpy as jnp
from jax import lax
from jax.experimental import pallas as pl
from jax.experimental.pallas import tpu as pltpu
from jax.sharding import PartitionSpec as P

MODES = 256
STEPS = 2
LANES = 128
WIDE = 256
BATCH = 8

step_scale = 0.25
f32 = jnp.float32
bf16 = jnp.bfloat16
i32 = jnp.int32


def iota(shape, dim):
    return lax.broadcasted_iota(i32, shape, dim)


def dot(a, b):
    return lax.dot_general(a, b, (((1,), (0,)), ((), ())), preferred_element_type=f32)


def dot_nt(a, b):
    return lax.dot_general(a, b, (((1,), (1,)), ((), ())), preferred_element_type=f32)


def hot(mask):
    return jnp.where(mask, 1.0, 0.0).astype(bf16)


def split(x):
    high = x.astype(bf16)
    return high, (x - high.astype(f32)).astype(bf16)


def stacked(x):
    high, low = split(x)
    return jnp.concatenate([high, low], axis=0)


def folded(x):
    half = x.shape[0] // 2
    return x[:half] + x[half:]


def thirds(x):
    first = x.astype(bf16).astype(f32)
    second = (x - first).astype(bf16).astype(f32)
    return jnp.concatenate([first, second, x - first - second], axis=0)


def cos_sin(x):
    turns = jnp.floor(x * 0.6366197723675814 + 0.5)
    r = x - turns * 1.5703125 - turns * 4.837512969970703125e-4 - turns * 7.54978995489188216e-8
    z = r * r
    sine = ((-1.9515295891e-4 * z + 8.3321608736e-3) * z - 1.6666654611e-1) * z * r + r
    cosine = ((2.443315711809948e-5 * z - 1.388731625493765e-3) * z + 4.166664568298827e-2) * z * z
    cosine = cosine - 0.5 * z + 1.0
    quarter = turns.astype(i32)
    odd = (quarter & 1) == 1
    cosine, sine = jnp.where(odd, sine, cosine), jnp.where(odd, cosine, sine)
    return (
        jnp.where(((quarter + 1) & 2) == 2, -cosine, cosine),
        jnp.where((quarter & 2) == 2, -sine, sine),
    )


def running(mask):
    rows, width = mask.shape
    below = hot(iota((LANES, LANES), 0) < iota((LANES, LANES), 1))
    total = jnp.zeros((rows, 1), f32)
    counts = []
    for start in range(0, width, LANES):
        block = mask[:, start : start + LANES]
        counts.append(dot(block.astype(bf16), below) + total)
        total = total + jnp.sum(block, axis=1, keepdims=True)
    return jnp.concatenate(counts, axis=1), total


def group_kernel(parts, copies, slot_hbm, *refs):
    fields, refs = refs[:6], refs[6:]
    out_ref, part_hbm, rank_hbm, part_ref, rank_ref, slot_ref, stack_ref, done = refs
    nodes = slot_ref.shape[1]
    per = nodes // parts
    stack_ref[...] = jnp.zeros_like(stack_ref)
    moves = [pltpu.make_async_copy(slot_hbm, slot_ref, done.at[0])]
    for index, field in enumerate(fields):
        moves.append(
            pltpu.make_async_copy(field, stack_ref.at[index + 1 : index + 2, :], done.at[index + 1])
        )
    for move in moves:
        move.start()
    moves[0].wait()
    slot = slot_ref[...].astype(f32)
    place = jnp.floor((slot + 0.5) * (1.0 / parts))
    part = (slot - place * parts).astype(i32)
    rows = max(16, parts)
    mask = jnp.where(iota((rows, nodes), 0) == part, 1.0, 0.0)
    count, _ = running(mask)
    rank = jnp.sum(mask * count, axis=0, keepdims=True).astype(i32)
    part_ref[...] = part
    rank_ref[...] = rank
    kept = [
        pltpu.make_async_copy(part_ref, part_hbm, done.at[7]),
        pltpu.make_async_copy(rank_ref, rank_hbm, done.at[8]),
    ]
    for move in kept:
        move.start()
    for move in moves[1:]:
        move.wait()
    stack_ref[0:1, :] = place
    terms = thirds(stack_ref[...])
    blocks = [jnp.where(part == index, terms, 0.0) for index in range(parts)]
    chosen = hot(iota((per, nodes), 0) == rank)
    moved = dot_nt(jnp.concatenate(blocks, axis=0).astype(bf16), chosen)
    for index in range(parts):
        block = moved[24 * index : 24 * index + 24]
        block = block[0:8] + block[8:16] + block[16:24]
        for copy in range(copies):
            out_ref[index * copies + copy] = block
    for move in kept:
        move.wait()


def ungroup_kernel(part_ref, rank_ref, value_ref, out_ref):
    parts, per = value_ref.shape
    nodes = part_ref.shape[1]
    chosen = hot(iota((per, nodes), 0) == rank_ref[...])
    back = dot(thirds(value_ref[...]).astype(bf16), chosen)
    back = back[0:parts] + back[parts : 2 * parts] + back[2 * parts :]
    mask = iota((parts, nodes), 0) == part_ref[...]
    out_ref[...] = jnp.sum(jnp.where(mask, back, 0.0), axis=0, keepdims=True)


def order_rows(
    elements, target_ref, rows_ref, lower_ref, upper_ref, key_ref, keycol_ref, off_ref, cnt_ref, win_ref
):
    blocks = off_ref.shape[0]
    count = target_ref.shape[1]
    shared = lower_ref.shape[1]
    mask = jnp.where(iota((blocks, count), 0) == target_ref[...], 1.0, 0.0)
    before, total = running(mask)
    totals = jnp.broadcast_to(total, (blocks, LANES))
    offset = dot(hot(iota((blocks, blocks), 1) < iota((blocks, blocks), 0)), totals.astype(bf16))
    off_ref[...] = offset
    cnt_ref[...] = totals
    window = jnp.floor(offset * (1.0 / LANES)) * LANES
    win_ref[...] = jnp.minimum(window, count - WIDE).astype(i32)
    place = jnp.sum(mask * (before + offset[:, 0:1]), axis=0, keepdims=True)
    strip = jnp.floor((place + 0.5) * (1.0 / LANES))
    lane = (place - strip * LANES).astype(i32)
    row = rows_ref[...].astype(f32)
    node = jnp.floor((row + 0.5) * (1.0 / elements))
    strips = count // LANES
    chosen = iota((strips, count), 0) == strip.astype(i32)
    terms = jnp.concatenate(
        [jnp.where(chosen, node, 0.0), jnp.where(chosen, row - node * elements, 0.0)], axis=0
    )
    moved = dot_nt(terms.astype(bf16), hot(iota((LANES, count), 0) == lane))
    moved = (moved[:strips] * elements + moved[strips:]).astype(i32)
    for index in range(strips):
        key_ref[:, index * LANES : (index + 1) * LANES] = moved[index : index + 1]
    key_ref[:, count : count + shared] = lower_ref[...]
    key_ref[:, count + shared : count + 2 * shared] = upper_ref[...]
    for start in range(0, count + 2 * shared, LANES):
        block = jnp.broadcast_to(key_ref[:, start : start + LANES].astype(f32), (LANES, LANES))
        keycol_ref[start : start + LANES, :] = block.T.astype(i32)


def fill_stack(value_ref, stack_ref):
    nodes, columns, elements = value_ref.shape
    for node in range(nodes):
        high, low = split(value_ref[node])
        lanes = slice(node * elements, (node + 1) * elements)
        stack_ref[0:columns, lanes] = high
        stack_ref[columns:, lanes] = low
    if stack_ref.shape[1] > nodes * elements:
        tail = slice(nodes * elements, stack_ref.shape[1])
        stack_ref[:, tail] = jnp.zeros_like(stack_ref[:, tail])


def picked(stack_ref, hot_ref, key_ref, start):
    depth = stack_ref.shape[1]
    key = key_ref[:, pl.ds(start, WIDE)]
    base = iota((LANES, WIDE), 0)
    for row in range(0, depth, LANES):
        hot_ref[row : row + LANES, :] = hot(base == key - row)
    return dot(stack_ref[...], hot_ref[0:depth, :])


def pick_rows(stack_ref, hot_ref, key_ref, out_ref):
    def body(index, carry):
        start = pl.multiple_of(index * WIDE, WIDE)
        out_ref[:, pl.ds(start, WIDE)] = picked(stack_ref, hot_ref, key_ref, start).astype(bf16)
        return carry

    lax.fori_loop(0, out_ref.shape[1] // WIDE, body, 0)


def pick_boundary(stack_ref, hot_ref, key_ref, low_ref, high_ref):
    shared = low_ref.shape[1]
    first = key_ref.shape[1] - 2 * shared
    for ref, origin in ((low_ref, first), (high_ref, first + shared)):
        for start in range(0, shared, WIDE):
            ref[:, start : start + WIDE] = folded(
                picked(stack_ref, hot_ref, key_ref, origin + start)
            )


def spread(derivative_ref, transposed, rows):
    nodes = derivative_ref.shape[0]
    size = 8 * nodes
    left = jnp.where(iota((rows, nodes), 0) // 8 == iota((rows, nodes), 1), 1.0, 0.0)
    right = jnp.where(iota((nodes, size), 1) // 8 == iota((nodes, size), 0), 1.0, 0.0)
    dims = (((1,), (1,)), ((), ())) if transposed else (((1,), (0,)), ((), ()))
    half = lax.dot_general(
        left, derivative_ref[...], dims, precision=lax.Precision.HIGHEST, preferred_element_type=f32
    )
    full = jnp.dot(half, right, precision=lax.Precision.HIGHEST, preferred_element_type=f32)
    full = jnp.where(iota((rows, size), 0) % 8 == iota((rows, size), 1) % 8, full, 0.0)
    return stacked(full)


def force_into(value_ref, forward, backward, radial_ref, shear_ref, first_order, force_ref):
    nodes, columns, elements = value_ref.shape
    size = 8 * nodes
    rows = forward.shape[0] // 2
    radial = jnp.broadcast_to(radial_ref[...][:, None, :], (nodes, 8, elements)).reshape(
        size, elements
    )
    radial = jnp.concatenate([radial, radial], axis=1)
    shear = jnp.broadcast_to(shear_ref[...][:, None, :], (nodes, 8, elements))

    def applied(matrix, x):
        high, low = split(x)
        both = dot(matrix[...], high)
        return both[:size] + both[rows : rows + size] + dot(matrix[0:rows, :], low)[:size]

    def body(index, carry):
        first = pl.multiple_of(index * 32, 32)
        starts = [first, first + 16]
        halves = [
            [value_ref[:, pl.ds(start, 8), :], value_ref[:, pl.ds(start + 8, 8), :]]
            for start in starts
        ]
        fields = [
            jnp.concatenate([half.reshape(size, elements) for half in pair], axis=1)
            for pair in halves
        ]
        fluxes = [radial * applied(forward, x) for x in fields]
        backs = [applied(backward, flux) for flux in fluxes]
        for start, pair, back in zip(starts, halves, backs):
            for side, half in enumerate(pair):
                order = (first_order + start + 8 * side + iota((8, elements), 0)).astype(f32)
                wave = (2.0 * order / MODES) ** 2
                block = back[:, side * elements : (side + 1) * elements]
                force_ref[:, pl.ds(start + 8 * side, 8), :] = (
                    -block.reshape(nodes, 8, elements) - shear * wave[None] * half
                )
        return carry

    lax.fori_loop(0, columns // 32, body, 0)


def transfers(pairs, done):
    return [
        pltpu.make_async_copy(source, target, done.at[index])
        for index, (source, target) in enumerate(pairs)
    ]


def begin(moves):
    for move in moves:
        move.start()


def finish(moves):
    for move in moves:
        move.wait()


def start_kernel(
    elements, box_ref, target_hbm, rows_hbm, lower_hbm, upper_hbm, derivative_hbm,
    value_hbm, radial_hbm, shear_hbm,
    off_ref, cnt_ref, win_ref, picked_ref,
    key_hbm, keycol_hbm, forward_hbm, backward_hbm, force_hbm, low_hbm, high_hbm,
    target_ref, rows_ref, lower_ref, upper_ref, derivative_ref, value_ref, radial_ref, shear_ref,
    key_ref, keycol_ref, forward_ref, backward_ref, force_ref, low_ref, high_ref,
    stack_ref, hot_ref, done, kept,
):
    moves = transfers(
        [
            (target_hbm, target_ref), (rows_hbm, rows_ref), (lower_hbm, lower_ref),
            (upper_hbm, upper_ref), (derivative_hbm, derivative_ref), (value_hbm, value_ref),
            (radial_hbm, radial_ref), (shear_hbm, shear_ref),
        ],
        done,
    )
    saves = transfers(
        [
            (key_ref, key_hbm), (keycol_ref, keycol_hbm), (forward_ref, forward_hbm),
            (backward_ref, backward_hbm), (force_ref, force_hbm), (low_ref, low_hbm),
            (high_ref, high_hbm),
        ],
        kept,
    )
    begin(moves)
    finish(moves[:5])
    order_rows(
        elements, target_ref, rows_ref, lower_ref, upper_ref, key_ref, keycol_ref, off_ref,
        cnt_ref, win_ref,
    )
    columns = value_ref.shape[1]
    rows = forward_ref.shape[0] // 2
    forward_ref[...] = spread(derivative_ref, False, rows)
    backward_ref[...] = spread(derivative_ref, True, rows)
    begin(saves[:4])
    finish(moves[5:])
    force_into(
        value_ref, forward_ref, backward_ref, radial_ref, shear_ref,
        box_ref[0] * columns % MODES, force_ref,
    )
    begin(saves[4:5])
    fill_stack(force_ref, stack_ref)
    pick_boundary(stack_ref, hot_ref, key_ref, low_ref, high_ref)
    begin(saves[5:])
    fill_stack(value_ref, stack_ref)
    pick_rows(stack_ref, hot_ref, key_ref, picked_ref)
    finish(saves)


def window_hot(win_ref, place_ref, group, stride):
    window = pl.multiple_of(win_ref[group * stride, 0], LANES)
    place = place_ref[pl.ds(group, 1), :]
    return window, hot(iota((WIDE, LANES), 0) + window == place)


def sample_into(win_ref, place_ref, harmonic_ref, picked_ref, stride, sample_ref):
    def body(index, carry):
        for group in [BATCH * index + part for part in range(BATCH)]:
            window, chosen = window_hot(win_ref, place_ref, group, stride)
            rows = folded(dot(picked_ref[:, pl.ds(window, WIDE)], chosen))
            sample_ref[pl.ds(group, 1), :] = jnp.sum(
                rows * harmonic_ref[group], axis=0, keepdims=True
            )
        return carry

    lax.fori_loop(0, sample_ref.shape[0] // BATCH, body, 0)


def node_kernel(
    stride, box_ref, win_ref, message_ref, off_ref, cnt_ref, picked_ref,
    harmonic_ref, place_ref, node_ref, sample_ref,
    near_re, near_im, far_re, far_im,
):
    groups, columns, _ = harmonic_ref.shape
    place = message_ref[:, 0, :]
    angle = message_ref[:, 1, :]
    place_ref[...] = jnp.where(place < cnt_ref[...], off_ref[...] + place, -1.0).astype(i32)
    for index in range(5):
        node_ref[index] = message_ref[:, 2 + index, :]

    def power(order):
        return cos_sin(order * angle)

    def times(x, y):
        return x[0] * y[0] - x[1] * y[1], x[0] * y[1] + x[1] * y[0]

    near = [(jnp.ones_like(angle), jnp.zeros_like(angle))] + [None] * 7
    for bit in (1, 2, 4):
        factor = power(float(bit))
        near[bit] = factor
        for low in range(1, bit):
            near[bit + low] = times(factor, near[low])
    for index, (re, im) in enumerate(near):
        near_re[:, index, :] = re
        near_im[:, index, :] = im
    first = box_ref[0] * columns
    base_re, base_im = power((first % MODES).astype(f32))
    sine = first >= MODES
    far = [
        (jnp.where(sine, base_im, base_re), jnp.where(sine, -base_re, base_im))
    ] + [None] * (columns // 8 - 1)
    bit = 1
    while bit < columns // 8:
        factor = power(float(8 * bit))
        for low in range(min(bit, columns // 8 - bit)):
            far[bit + low] = times(factor, far[low])
        bit *= 2
    for index, (re, im) in enumerate(far):
        far_re[index] = re
        far_im[index] = im

    def body(group, carry):
        re, im = near_re[group], near_im[group]
        for index in range(columns // 8):
            harmonic_ref[group, 8 * index : 8 * index + 8, :] = (
                far_re[index, pl.ds(group, 1), :] * re - far_im[index, pl.ds(group, 1), :] * im
            )
        return carry

    lax.fori_loop(0, groups, body, 0)
    sample_into(win_ref, place_ref, harmonic_ref, picked_ref, stride, sample_ref)


def nodes_step(samples_ref, node_ref, now, before, next_ref, coefficient_ref):
    sample = samples_ref[0]
    for index in range(1, samples_ref.shape[0]):
        sample = sample + samples_ref[index]
    pull = node_ref[0] * (sample - now)
    next_ref[...] = 2.0 * now - before + step_scale * pull / node_ref[1]
    coefficient_ref[...] = -node_ref[2] * pull


def annulus_step(
    early, late, emit, stride, first_order, win_ref, place_ref, harmonic_ref, coefficient_ref, keycol_ref,
    below_ref, above_ref, value_ref, previous_ref, force_ref, mass_ref, modes_ref,
    next_ref, reaction_ref, terms_ref, hot_ref, hot2_ref, added_ref,
):
    nodes, columns, elements = value_ref.shape
    groups = place_ref.shape[0]
    count = reaction_ref.shape[1]
    shared = below_ref.shape[1]
    reaction_ref[...] = jnp.zeros_like(reaction_ref)

    def react(index, carry):
        found = []
        for group in [BATCH * index + part for part in range(BATCH)]:
            window, chosen = window_hot(win_ref, place_ref, group, stride)
            weighted = harmonic_ref[group] * coefficient_ref[pl.ds(group, 1), :]
            found.append((window, folded(dot_nt(stacked(weighted), chosen))))
        for window, rows in found:
            reaction_ref[:, pl.ds(window, WIDE)] = reaction_ref[:, pl.ds(window, WIDE)] + rows
        return carry

    lax.fori_loop(0, groups // BATCH, react, 0)
    finish(early)
    terms_ref[:, 0:count] = stacked(reaction_ref[...])
    terms_ref[:, count : count + shared] = stacked(below_ref[...])
    terms_ref[:, count + shared : count + 2 * shared] = stacked(above_ref[...])
    depth = count + 2 * shared
    lane = iota((LANES, LANES), 1)

    def place_rows(first, width, buffer):
        for side in range(width):
            base = lane + (first + side) * elements
            for row in range(0, depth, LANES):
                buffer[row : row + LANES, side * LANES : (side + 1) * LANES] = hot(
                    keycol_ref[row : row + LANES, :] == base
                )
        rows = folded(dot(terms_ref[...], buffer[0:depth, 0 : width * LANES]))
        for side in range(width):
            added_ref[first + side] = rows[:, side * LANES : (side + 1) * LANES]

    def place_four(index, carry):
        place_rows(4 * index, 2, hot_ref)
        place_rows(4 * index + 2, 2, hot2_ref)
        return carry

    lax.fori_loop(0, nodes // 4, place_four, 0)
    for first in range(nodes // 4 * 4, nodes, 2):
        place_rows(first, min(2, nodes - first), hot_ref)
    order = first_order + iota((columns, elements), 0)
    finish(late)
    live = order < modes_ref[...]
    for node in range(nodes):
        gain = jnp.where(live, step_scale / mass_ref[node : node + 1, :], 0.0)
        next_ref[node] = (
            2.0 * value_ref[node]
            - previous_ref[node]
            + gain * (force_ref[node] + added_ref[node])
        )
        emit(node)


def middle_kernel(
    stride, box_ref, win_ref, samples_ref, node_ref, place_ref, harmonic_ref,
    keycol_hbm, below_hbm, above_hbm, value_hbm, previous_hbm, force_hbm, mass_hbm, modes_hbm,
    key_hbm, forward_hbm, backward_hbm, radial_hbm, shear_hbm,
    sample_ref, boxnext_ref, next_hbm, nextforce_hbm, low_hbm, high_hbm,
    keycol_ref, below_ref, above_ref, value_ref, previous_ref, force_ref, mass_ref, modes_ref,
    key_ref, forward_ref, backward_ref, radial_ref, shear_ref,
    next_ref, low_ref, high_ref,
    coefficient_ref, reaction_ref, terms_ref, hot_ref, hot2_ref, added_ref, stack_ref, picked_ref,
    done, kept,
):
    moves = transfers(
        [
            (keycol_hbm, keycol_ref), (below_hbm, below_ref), (above_hbm, above_ref),
            (value_hbm, value_ref), (previous_hbm, previous_ref), (force_hbm, force_ref),
            (mass_hbm, mass_ref), (modes_hbm, modes_ref), (key_hbm, key_ref),
            (forward_hbm, forward_ref), (backward_hbm, backward_ref), (radial_hbm, radial_ref),
            (shear_hbm, shear_ref),
        ],
        done,
    )
    saves = transfers(
        [
            (next_ref, next_hbm), (added_ref, nextforce_hbm), (low_ref, low_hbm),
            (high_ref, high_hbm),
        ],
        kept,
    )
    begin(moves)
    columns = value_ref.shape[1]
    first_order = box_ref[0] * columns % MODES
    nodes_step(samples_ref, node_ref, node_ref[3], node_ref[4], boxnext_ref, coefficient_ref)
    annulus_step(
        moves[:3], moves[3:], lambda node: None,
        stride, first_order, win_ref, place_ref, harmonic_ref, coefficient_ref, keycol_ref,
        below_ref, above_ref, value_ref, previous_ref, force_ref, mass_ref, modes_ref,
        next_ref, reaction_ref, terms_ref, hot_ref, hot2_ref, added_ref,
    )
    begin(saves[:1])
    force_into(
        next_ref, forward_ref, backward_ref, radial_ref, shear_ref, first_order, added_ref
    )
    begin(saves[1:2])
    fill_stack(added_ref, stack_ref)
    pick_boundary(stack_ref, hot_ref, key_ref, low_ref, high_ref)
    begin(saves[2:])
    fill_stack(next_ref, stack_ref)
    pick_rows(stack_ref, hot_ref, key_ref, picked_ref)
    sample_into(win_ref, place_ref, harmonic_ref, picked_ref, stride, sample_ref)
    finish(saves)


def box_kernel(samples_ref, node_ref, now_ref, boxnext_ref, coefficient_ref):
    nodes_step(samples_ref, node_ref, now_ref[...], node_ref[3], boxnext_ref, coefficient_ref)


def last_kernel(
    stride, box_ref, win_ref, coefficient_ref, place_ref, harmonic_ref,
    keycol_hbm, below_hbm, above_hbm, value_hbm, previous_hbm, force_hbm, mass_hbm, modes_hbm,
    next_hbm,
    keycol_ref, below_ref, above_ref, value_ref, previous_ref, force_ref, mass_ref, modes_ref,
    next_ref, reaction_ref, terms_ref, hot_ref, hot2_ref, added_ref, done, kept,
):
    moves = transfers(
        [
            (keycol_hbm, keycol_ref), (below_hbm, below_ref), (above_hbm, above_ref),
            (value_hbm, value_ref), (previous_hbm, previous_ref), (force_hbm, force_ref),
            (mass_hbm, mass_ref), (modes_hbm, modes_ref),
        ],
        done,
    )
    begin(moves)
    first_order = box_ref[0] * value_ref.shape[1] % MODES
    saves = transfers(
        [(next_ref.at[node], next_hbm.at[node]) for node in range(value_ref.shape[0])], kept
    )
    annulus_step(
        moves[:3], moves[3:], lambda node: saves[node].start(),
        stride, first_order, win_ref, place_ref, harmonic_ref, coefficient_ref, keycol_ref,
        below_ref, above_ref, value_ref, previous_ref, force_ref, mass_ref, modes_ref,
        next_ref, reaction_ref, terms_ref, hot_ref, hot2_ref, added_ref,
    )
    finish(saves)


def exchanged(low, high):
    size = lax.axis_size("mer")
    up = [(i, i + 1) for i in range(size - 1)]
    down = [(j, i) for i, j in up]
    return lax.ppermute(high, "mer", up), lax.ppermute(low, "mer", down)


SMEM, VMEM, HBM = pltpu.SMEM, pltpu.VMEM, pltpu.HBM


def call(kernel, ins, outs, scratch=(), copies=(), name=None, limit=40):
    arrays = [
        pltpu.with_memory_space_constraint(array, memory) if pinned else array
        for array, memory, pinned in ins
    ]
    return pl.pallas_call(
        kernel,
        out_shape=[
            memory(shape, dtype) if memory else jax.ShapeDtypeStruct(shape, dtype)
            for shape, dtype, memory in outs
        ],
        in_specs=[pl.BlockSpec(memory_space=memory) for _, memory, _ in ins],
        out_specs=[pl.BlockSpec(memory_space=memory or VMEM) for _, _, memory in outs],
        scratch_shapes=[VMEM(shape, dtype) for shape, dtype in scratch]
        + [pltpu.SemaphoreType.DMA((number,)) for number in copies],
        compiler_params=pltpu.CompilerParams(vmem_limit_bytes=limit << 20),
        name=name,
    )(*arrays)


def per_device(
    annulus,
    annulus_prev,
    derivative,
    radial_modulus,
    shear_modulus,
    node_mass,
    element_modes,
    upper_rows,
    lower_rows,
    coupling_rows,
    coupling_target,
    box_field,
    box_prev,
    box_angle,
    box_spring,
    box_mass,
    box_weight,
    box_slot,
):
    mer_count = lax.axis_size("mer")
    box_count = lax.axis_size("box")
    blocks = mer_count * box_count
    nodes, columns, elements = annulus.shape
    box_nodes = box_slot.shape[0]
    per = box_nodes // mer_count
    stride = LANES // per
    groups = blocks * per // LANES
    count = coupling_rows.shape[0]
    shared = upper_rows.shape[0]
    depth = count + 2 * shared
    padded_nodes = nodes + nodes % 2
    rows = -(-8 * nodes // 16) * 16
    volume = (nodes, columns, elements)
    grid = (groups, LANES)
    flat = (nodes, elements)
    hot_scratch = ((max(padded_nodes * elements, depth), WIDE), bf16)
    stack_scratch = ((2 * columns, padded_nodes * elements), bf16)

    def far(value):
        return value, HBM, True

    def near(value):
        return value, VMEM, True

    def landed(value):
        return value, VMEM, False

    def anywhere(value):
        return value, pl.ANY, False

    def scalar(value):
        return value, SMEM, False

    box = scalar(jnp.full((1,), lax.axis_index("box"), i32))

    sent = [
        far(value.reshape(1, box_nodes))
        for value in (box_slot, box_angle, box_spring, box_mass, box_weight, box_field, box_prev)
    ]
    line = ((1, box_nodes), i32)
    messages, part, rank = call(
        functools.partial(group_kernel, mer_count, box_count),
        sent,
        [((blocks, 8, per), f32, None), line + (HBM,), line + (HBM,)],
        [line, line, line, ((8, box_nodes), f32)],
        copies=(9,),
        name="group",
    )
    messages = lax.all_to_all(messages, ("mer", "box"), split_axis=0, concat_axis=0, tiled=True)
    if stride > 1:
        messages = messages.reshape(groups, stride, 8, per).swapaxes(1, 2)
        messages = messages.reshape(groups, 8, LANES)

    expanded = VMEM if stride == 1 else None
    field = (volume, f32)
    table = (flat, f32)
    limits = ((1, elements), i32)
    side = ((columns, shared), f32)
    keys = [((1, depth), i32), ((depth, LANES), i32)]
    matrices = [((2 * rows, 8 * nodes), bf16)] * 2
    picked = ((2 * columns, count), bf16)
    kept = keys + matrices + [field, side, side]
    (
        offset, filled, window, chosen, key, keycol, forward, backward, force, low, high,
    ) = call(
        functools.partial(start_kernel, elements),
        [
            box,
            far(coupling_target.reshape(1, count)),
            far(coupling_rows.reshape(1, count)),
            far(lower_rows.reshape(1, shared)),
            far(upper_rows.reshape(1, shared)),
            far(derivative),
            far(annulus),
            far(radial_modulus),
            far(shear_modulus),
        ],
        [
            ((blocks, LANES), f32, expanded),
            ((blocks, LANES), f32, expanded),
            ((blocks, LANES), i32, None),
            picked + (VMEM,),
        ]
        + [shape + (HBM,) for shape in kept],
        [((1, count), i32)] * 2
        + [((1, shared), i32)] * 2
        + [((nodes, nodes), f32), field, table, table]
        + kept
        + [stack_scratch, hot_scratch],
        copies=(8, 7),
        name="start",
    )
    if stride > 1:
        offset = landed(jnp.repeat(offset[:, 0], per).reshape(groups, LANES))
        filled = landed(jnp.repeat(filled[:, 0], per).reshape(groups, LANES))
    else:
        offset, filled = near(offset), near(filled)
    window = scalar(window)
    below, above = exchanged(low, high)

    harmonic, place, node, sample = call(
        functools.partial(node_kernel, stride),
        [box, window, landed(messages), offset, filled, near(chosen)],
        [
            ((groups, columns, LANES), f32, VMEM),
            (grid, i32, VMEM),
            ((5, groups, LANES), f32, VMEM),
            (grid, f32, None),
        ],
        [((groups, 8, LANES), f32)] * 2 + [((columns // 8, groups, LANES), f32)] * 2,
        name="nodes",
    )
    samples = lax.all_gather(sample, "box")

    modes = element_modes.reshape(1, elements)
    fetched = keys[1:] + [side, side, field, field, field, table, limits]
    step_scratch = [
        ((columns, count), f32),
        ((2 * columns, depth), bf16),
        hot_scratch,
        hot_scratch,
        field,
    ]
    sample, box_now, current, force, low, high = call(
        functools.partial(middle_kernel, stride),
        [
            box, window, landed(samples), near(node), near(place), near(harmonic),
            far(keycol), anywhere(below), anywhere(above), far(annulus), far(annulus_prev), far(force),
            far(node_mass), far(modes), far(key), far(forward), far(backward),
            far(radial_modulus), far(shear_modulus),
        ],
        [(grid, f32, None), (grid, f32, VMEM)]
        + [shape + (HBM,) for shape in (field, field, side, side)],
        fetched
        + keys[:1]
        + matrices
        + [table, table, field, side, side]
        + [(grid, f32)]
        + step_scratch
        + [stack_scratch, picked],
        copies=(13, 4),
        name="middle",
    )
    below, above = exchanged(low, high)
    samples = lax.all_gather(sample, "box")

    box_now, coefficient = call(
        box_kernel,
        [landed(samples), near(node), near(box_now)],
        [(grid, f32, None), (grid, f32, VMEM)],
        name="box",
    )
    returned = lax.all_to_all(
        box_now.reshape(mer_count, box_count, per), "mer", split_axis=0, concat_axis=0, tiled=True
    )
    returned = lax.dynamic_index_in_dim(
        returned, lax.axis_index("box"), axis=1, keepdims=False
    )
    (box_out,) = call(
        ungroup_kernel,
        [landed(part), landed(rank), landed(returned)],
        [((1, box_nodes), f32, None)],
        name="ungroup",
    )
    (current,) = call(
        functools.partial(last_kernel, stride),
        [
            box, window, near(coefficient), near(place), near(harmonic), far(keycol),
            anywhere(below), anywhere(above), far(current), far(annulus), far(force), far(node_mass), far(modes),
        ],
        [field + (HBM,)],
        fetched + [field] + step_scratch,
        copies=(8, nodes),
        name="last",
    )
    return current, box_out.reshape(box_nodes)


def solution(mesh):
    in_specs = (
        P(None, "box", "mer"),
        P(None, "box", "mer"),
        P(),
        P(None, "mer"),
        P(None, "mer"),
        P(None, "mer"),
        P("mer"),
        P("mer"),
        P("mer"),
        P("mer"),
        P("mer", None),
        P(("mer", "box")),
        P(("mer", "box")),
        P(("mer", "box")),
        P(("mer", "box")),
        P(("mer", "box")),
        P(("mer", "box")),
        P(("mer", "box")),
    )
    out_specs = (P(None, "box", "mer"), P(("mer", "box")))
    return jax.shard_map(
        per_device, mesh=mesh, in_specs=in_specs, out_specs=out_specs, check_vma=False
    )
```

```python
import functools

import jax
import jax.numpy as jnp
from jax import lax
from jax.experimental import pallas as pl
from jax.experimental.pallas import tpu as pltpu
from jax.sharding import PartitionSpec as P

MODES = 256
STEPS = 2
LANES = 128
WIDE = 256
BATCH = 16
PAIRS = 6
CHAINS = 4

step_scale = 0.25
f32 = jnp.float32
bf16 = jnp.bfloat16
i32 = jnp.int32


def iota(shape, dim):
    return lax.broadcasted_iota(i32, shape, dim)


def dot(a, b):
    return lax.dot_general(a, b, (((1,), (0,)), ((), ())), preferred_element_type=f32)


def dot_nt(a, b):
    return lax.dot_general(a, b, (((1,), (1,)), ((), ())), preferred_element_type=f32)


def hot(mask):
    return jnp.where(mask, 1.0, 0.0).astype(bf16)


def split(x):
    high = x.astype(bf16)
    return high, (x - high.astype(f32)).astype(bf16)


def stacked(x):
    high, low = split(x)
    return jnp.concatenate([high, low], axis=0)


def folded(x):
    half = x.shape[0] // 2
    return x[:half] + x[half:]


def thirds(x):
    first = x.astype(bf16).astype(f32)
    second = (x - first).astype(bf16).astype(f32)
    return jnp.concatenate([first, second, x - first - second], axis=0)


def cos_sin(x):
    turns = jnp.floor(x * 0.6366197723675814 + 0.5)
    r = x - turns * 1.5703125 - turns * 4.837512969970703125e-4 - turns * 7.54978995489188216e-8
    z = r * r
    sine = ((-1.9515295891e-4 * z + 8.3321608736e-3) * z - 1.6666654611e-1) * z * r + r
    cosine = ((2.443315711809948e-5 * z - 1.388731625493765e-3) * z + 4.166664568298827e-2) * z * z
    cosine = cosine - 0.5 * z + 1.0
    quarter = turns.astype(i32)
    odd = (quarter & 1) == 1
    cosine, sine = jnp.where(odd, sine, cosine), jnp.where(odd, cosine, sine)
    return (
        jnp.where(((quarter + 1) & 2) == 2, -cosine, cosine),
        jnp.where((quarter & 2) == 2, -sine, sine),
    )


def running(mask):
    rows, width = mask.shape
    below = hot(iota((LANES, LANES), 0) < iota((LANES, LANES), 1))
    total = jnp.zeros((rows, 1), f32)
    counts = []
    for start in range(0, width, LANES):
        block = mask[:, start : start + LANES]
        counts.append(dot(block.astype(bf16), below) + total)
        total = total + jnp.sum(block, axis=1, keepdims=True)
    return jnp.concatenate(counts, axis=1), total


def group_kernel(parts, copies, slot_hbm, *refs):
    fields, refs = refs[:6], refs[6:]
    out_ref, part_hbm, rank_hbm, part_ref, rank_ref, slot_ref, stack_ref, done = refs
    nodes = slot_ref.shape[1]
    per = nodes // parts
    stack_ref[...] = jnp.zeros_like(stack_ref)
    moves = [pltpu.make_async_copy(slot_hbm, slot_ref, done.at[0])]
    for index, field in enumerate(fields):
        moves.append(
            pltpu.make_async_copy(field, stack_ref.at[index + 1 : index + 2, :], done.at[index + 1])
        )
    for move in moves:
        move.start()
    moves[0].wait()
    slot = slot_ref[...].astype(f32)
    place = jnp.floor((slot + 0.5) * (1.0 / parts))
    part = (slot - place * parts).astype(i32)
    rows = max(16, parts)
    mask = jnp.where(iota((rows, nodes), 0) == part, 1.0, 0.0)
    count, _ = running(mask)
    rank = jnp.sum(mask * count, axis=0, keepdims=True).astype(i32)
    part_ref[...] = part
    rank_ref[...] = rank
    kept = [
        pltpu.make_async_copy(part_ref, part_hbm, done.at[7]),
        pltpu.make_async_copy(rank_ref, rank_hbm, done.at[8]),
    ]
    for move in kept:
        move.start()
    for move in moves[1:]:
        move.wait()
    stack_ref[0:1, :] = place
    terms = thirds(stack_ref[...])
    blocks = [jnp.where(part == index, terms, 0.0) for index in range(parts)]
    chosen = hot(iota((per, nodes), 0) == rank)
    moved = dot_nt(jnp.concatenate(blocks, axis=0).astype(bf16), chosen)
    for index in range(parts):
        block = moved[24 * index : 24 * index + 24]
        block = block[0:8] + block[8:16] + block[16:24]
        for copy in range(copies):
            out_ref[index * copies + copy] = block
    for move in kept:
        move.wait()


def ungroup_kernel(part_ref, rank_ref, value_ref, out_ref):
    parts, per = value_ref.shape
    nodes = part_ref.shape[1]
    chosen = hot(iota((per, nodes), 0) == rank_ref[...])
    back = dot(thirds(value_ref[...]).astype(bf16), chosen)
    back = back[0:parts] + back[parts : 2 * parts] + back[2 * parts :]
    mask = iota((parts, nodes), 0) == part_ref[...]
    out_ref[...] = jnp.sum(jnp.where(mask, back, 0.0), axis=0, keepdims=True)


def order_rows(
    elements, target_ref, rows_ref, lower_ref, upper_ref, key_ref, keycol_ref, off_ref, cnt_ref, win_ref
):
    blocks = off_ref.shape[0]
    count = target_ref.shape[1]
    shared = lower_ref.shape[1]
    mask = jnp.where(iota((blocks, count), 0) == target_ref[...], 1.0, 0.0)
    before, total = running(mask)
    totals = jnp.broadcast_to(total, (blocks, LANES))
    offset = dot(hot(iota((blocks, blocks), 1) < iota((blocks, blocks), 0)), totals.astype(bf16))
    off_ref[...] = offset
    cnt_ref[...] = totals
    window = jnp.floor(offset * (1.0 / LANES)) * LANES
    win_ref[...] = jnp.minimum(window, count - WIDE).T[0:1, :].astype(i32)
    place = jnp.sum(mask * (before + offset[:, 0:1]), axis=0, keepdims=True)
    strip = jnp.floor((place + 0.5) * (1.0 / LANES))
    lane = (place - strip * LANES).astype(i32)
    row = rows_ref[...].astype(f32)
    node = jnp.floor((row + 0.5) * (1.0 / elements))
    strips = count // LANES
    chosen = iota((strips, count), 0) == strip.astype(i32)
    terms = jnp.concatenate(
        [jnp.where(chosen, node, 0.0), jnp.where(chosen, row - node * elements, 0.0)], axis=0
    )
    moved = dot_nt(terms.astype(bf16), hot(iota((LANES, count), 0) == lane))
    moved = (moved[:strips] * elements + moved[strips:]).astype(i32)
    for index in range(strips):
        key_ref[:, index * LANES : (index + 1) * LANES] = moved[index : index + 1]
    key_ref[:, count : count + shared] = lower_ref[...]
    key_ref[:, count + shared : count + 2 * shared] = upper_ref[...]
    for start in range(0, count + 2 * shared, LANES):
        block = jnp.broadcast_to(key_ref[:, start : start + LANES].astype(f32), (LANES, LANES))
        keycol_ref[start : start + LANES, :] = block.T.astype(i32)


def fill_stack(value_ref, stack_ref):
    nodes, columns, elements = value_ref.shape
    for node in range(nodes):
        high, low = split(value_ref[node])
        lanes = slice(node * elements, (node + 1) * elements)
        stack_ref[0:columns, lanes] = high
        stack_ref[columns:, lanes] = low
    if stack_ref.shape[1] > nodes * elements:
        tail = slice(nodes * elements, stack_ref.shape[1])
        stack_ref[:, tail] = jnp.zeros_like(stack_ref[:, tail])


def picked(stack_ref, key_ref, start):
    key = key_ref[:, pl.ds(start, WIDE)]
    base = iota((LANES, WIDE), 0)
    chosen = [hot(base == key - row) for row in range(0, stack_ref.shape[1], LANES)]
    return dot(stack_ref[...], jnp.concatenate(chosen, axis=0))


def pick_rows(stack_ref, key_ref, out_ref):
    def body(index, carry):
        for part in range(4):
            start = pl.multiple_of((4 * index + part) * WIDE, WIDE)
            out_ref[:, pl.ds(start, WIDE)] = picked(stack_ref, key_ref, start).astype(bf16)
        return carry

    lax.fori_loop(0, out_ref.shape[1] // (4 * WIDE), body, 0)


def pick_boundary(stack_ref, key_ref, low_ref, high_ref):
    shared = low_ref.shape[1]
    first = key_ref.shape[1] - 2 * shared
    for ref, origin in ((low_ref, first), (high_ref, first + shared)):
        for start in range(0, shared, WIDE):
            ref[:, start : start + WIDE] = folded(picked(stack_ref, key_ref, origin + start))


def spread(derivative_ref, transposed, rows):
    nodes = derivative_ref.shape[0]
    size = 8 * nodes
    left = hot(iota((rows, nodes), 0) // 8 == iota((rows, nodes), 1))
    right = hot(iota((nodes, size), 1) // 8 == iota((nodes, size), 0))
    same = iota((rows, size), 0) % 8 == iota((rows, size), 1) % 8
    parts = []
    for term in split(derivative_ref[...]):
        half = (dot_nt if transposed else dot)(left, term)
        parts.append(jnp.where(same, dot(half.astype(bf16), right), 0.0))
    return jnp.concatenate(parts, axis=0).astype(bf16)


def force_into(value_ref, forward, backward, radial_ref, shear_ref, first_order, force_ref):
    nodes, columns, elements = value_ref.shape
    size = 8 * nodes
    rows = forward.shape[0] // 2
    radial = jnp.broadcast_to(radial_ref[...][:, None, :], (nodes, 8, elements)).reshape(
        size, elements
    )
    radial = jnp.concatenate([radial, radial], axis=1)
    shear = jnp.broadcast_to(shear_ref[...][:, None, :], (nodes, 8, elements))

    def applied(matrix, x):
        high, low = split(x)
        both = dot(matrix[...], high)
        return both[:size] + both[rows : rows + size] + dot(matrix[0:rows, :], low)[:size]

    def body(index, carry):
        first = pl.multiple_of(index * 16 * CHAINS, 16 * CHAINS)
        starts = [first + 16 * chain for chain in range(CHAINS)]
        halves = [
            [value_ref[:, pl.ds(start, 8), :], value_ref[:, pl.ds(start + 8, 8), :]]
            for start in starts
        ]
        fields = [
            jnp.concatenate([half.reshape(size, elements) for half in pair], axis=1)
            for pair in halves
        ]
        fluxes = [radial * applied(forward, x) for x in fields]
        backs = [applied(backward, flux) for flux in fluxes]
        for start, pair, back in zip(starts, halves, backs):
            for side, half in enumerate(pair):
                order = (first_order + start + 8 * side + iota((8, elements), 0)).astype(f32)
                wave = (2.0 * order / MODES) ** 2
                block = back[:, side * elements : (side + 1) * elements]
                force_ref[:, pl.ds(start + 8 * side, 8), :] = (
                    -block.reshape(nodes, 8, elements) - shear * wave[None] * half
                )
        return carry

    lax.fori_loop(0, columns // (16 * CHAINS), body, 0)


def transfers(pairs, done):
    return [
        pltpu.make_async_copy(source, target, done.at[index])
        for index, (source, target) in enumerate(pairs)
    ]


def begin(moves):
    for move in moves:
        move.start()


def finish(moves):
    for move in moves:
        move.wait()


def start_kernel(
    elements, box_ref, target_hbm, rows_hbm, lower_hbm, upper_hbm, derivative_hbm,
    value_hbm, radial_hbm, shear_hbm,
    win_ref, off_hbm, cnt_hbm, picked_hbm, key_hbm, keycol_hbm, forward_hbm, backward_hbm, force_hbm, low_hbm, high_hbm,
    target_ref, rows_ref, lower_ref, upper_ref, derivative_ref, value_ref, radial_ref, shear_ref,
    off_ref, cnt_ref, picked_ref, key_ref, keycol_ref, forward_ref, backward_ref, force_ref, low_ref,
    high_ref, stack_ref, done, kept,
):
    moves = transfers(
        [
            (target_hbm, target_ref), (rows_hbm, rows_ref), (lower_hbm, lower_ref),
            (upper_hbm, upper_ref), (derivative_hbm, derivative_ref), (value_hbm, value_ref),
            (radial_hbm, radial_ref), (shear_hbm, shear_ref),
        ],
        done,
    )
    saves = transfers(
        [
            (off_ref, off_hbm), (cnt_ref, cnt_hbm), (picked_ref, picked_hbm),
            (key_ref, key_hbm), (keycol_ref, keycol_hbm), (forward_ref, forward_hbm),
            (backward_ref, backward_hbm), (force_ref, force_hbm), (low_ref, low_hbm),
            (high_ref, high_hbm),
        ],
        kept,
    )
    begin(moves)
    finish(moves[:5])
    order_rows(
        elements, target_ref, rows_ref, lower_ref, upper_ref, key_ref, keycol_ref, off_ref,
        cnt_ref, win_ref,
    )
    columns = value_ref.shape[1]
    rows = forward_ref.shape[0] // 2
    forward_ref[...] = spread(derivative_ref, False, rows)
    backward_ref[...] = spread(derivative_ref, True, rows)
    begin(saves[:2] + saves[3:7])
    finish(moves[5:])
    fill_stack(value_ref, stack_ref)
    pick_rows(stack_ref, key_ref, picked_ref)
    begin(saves[2:3])
    force_into(
        value_ref, forward_ref, backward_ref, radial_ref, shear_ref,
        box_ref[0] * columns % MODES, force_ref,
    )
    begin(saves[7:8])
    fill_stack(force_ref, stack_ref)
    pick_boundary(stack_ref, key_ref, low_ref, high_ref)
    begin(saves[8:])
    finish(saves)


def window_hot(win_ref, harmonic_ref, group, stride):
    window = pl.multiple_of(win_ref[0, group * stride], LANES)
    columns = harmonic_ref.shape[1] - 8
    place = harmonic_ref[group, columns : columns + 1, :].astype(i32)
    return window, hot(iota((WIDE, LANES), 0) + window == place)


def sample_into(win_ref, harmonic_ref, picked_ref, stride, sample_ref):
    columns = harmonic_ref.shape[1] - 8

    def body(index, carry):
        for group in [BATCH * index + part for part in range(BATCH)]:
            window, chosen = window_hot(win_ref, harmonic_ref, group, stride)
            rows = folded(dot(picked_ref[:, pl.ds(window, WIDE)], chosen))
            sample_ref[pl.ds(group, 1), :] = jnp.sum(
                rows * harmonic_ref[group, 0:columns, :], axis=0, keepdims=True
            )
        return carry

    lax.fori_loop(0, sample_ref.shape[0] // BATCH, body, 0)


def times(x, y):
    return x[0] * y[0] - x[1] * y[1], x[0] * y[1] + x[1] * y[0]


def node_kernel(
    stride, box_ref, win_ref, message_ref, off_hbm, cnt_hbm, picked_hbm,
    harmonic_ref, node_ref, sample_ref,
    off_ref, cnt_ref, picked_ref, place_ref, near_ref, far_re, far_im, done,
):
    moves = transfers(
        [(off_hbm, off_ref), (cnt_hbm, cnt_ref), (picked_hbm, picked_ref)], done
    )
    begin(moves)
    groups, columns = harmonic_ref.shape[0], harmonic_ref.shape[1] - 8
    place = message_ref[:, 0, :]
    angle = message_ref[:, 1, :]
    for index in range(5):
        node_ref[index] = message_ref[:, 2 + index, :]
    for bit in range(3):
        re, im = cos_sin(float(1 << bit) * angle)
        near_ref[2 * bit] = re
        near_ref[2 * bit + 1] = im
    first = box_ref[0] * columns
    base_re, base_im = cos_sin((first % MODES).astype(f32) * angle)
    sine = first >= MODES
    far = [
        (jnp.where(sine, base_im, base_re), jnp.where(sine, -base_re, base_im))
    ] + [None] * (columns // 8 - 1)
    bit = 1
    while bit < columns // 8:
        factor = cos_sin(float(8 * bit) * angle)
        for low in range(min(bit, columns // 8 - bit)):
            far[bit + low] = times(factor, far[low])
        bit *= 2
    for index, (re, im) in enumerate(far):
        far_re[index] = re
        far_im[index] = im
    finish(moves[:2])
    place_ref[...] = jnp.where(place < cnt_ref[...], off_ref[...] + place, -1.0)
    order = iota((8, LANES), 0)

    def body(index, carry):
        for group in [4 * index + part for part in range(4)]:
            row = pl.ds(group, 1)
            powers = [
                (
                    jnp.where((order >> bit) & 1 == 1, near_ref[2 * bit, row, :], 1.0),
                    jnp.where((order >> bit) & 1 == 1, near_ref[2 * bit + 1, row, :], 0.0),
                )
                for bit in range(3)
            ]
            re, im = times(times(powers[0], powers[1]), powers[2])
            for step in range(columns // 8):
                harmonic_ref[group, 8 * step : 8 * step + 8, :] = (
                    far_re[step, row, :] * re - far_im[step, row, :] * im
                )
            harmonic_ref[group, columns : columns + 8, :] = jnp.broadcast_to(
                place_ref[row, :], (8, LANES)
            )
        return carry

    lax.fori_loop(0, groups // 4, body, 0)
    finish(moves[2:])
    sample_into(win_ref, harmonic_ref, picked_ref, stride, sample_ref)


def nodes_step(samples_ref, node_ref, now, before, next_ref, coefficient_ref):
    sample = samples_ref[0]
    for index in range(1, samples_ref.shape[0]):
        sample = sample + samples_ref[index]
    pull = node_ref[0] * (sample - now)
    next_ref[...] = 2.0 * now - before + step_scale * pull / node_ref[1]
    coefficient_ref[...] = -node_ref[2] * pull


def react_into(win_ref, harmonic_ref, coefficient_ref, stride, reaction_ref):
    reaction_ref[...] = jnp.zeros_like(reaction_ref)
    columns = reaction_ref.shape[0]

    def react(index, carry):
        found = []
        for group in [BATCH * index + part for part in range(BATCH)]:
            window, chosen = window_hot(win_ref, harmonic_ref, group, stride)
            weighted = harmonic_ref[group, 0:columns, :] * coefficient_ref[pl.ds(group, 1), :]
            found.append((window, folded(dot_nt(stacked(weighted), chosen))))
        for window, rows in found:
            reaction_ref[:, pl.ds(window, WIDE)] = reaction_ref[:, pl.ds(window, WIDE)] + rows
        return carry

    lax.fori_loop(0, harmonic_ref.shape[0] // BATCH, react, 0)


def place_into(terms_ref, keycol_ref, elements, nodes, added_ref):
    depth = terms_ref.shape[1]
    lane = iota((LANES, LANES), 1)

    def place_rows(first, width):
        sides = []
        for side in range(width):
            base = lane + (first + side) * elements
            chosen = [
                hot(keycol_ref[row : row + LANES, :] == base) for row in range(0, depth, LANES)
            ]
            sides.append(jnp.concatenate(chosen, axis=0))
        rows = folded(dot(terms_ref[...], jnp.concatenate(sides, axis=1)))
        for side in range(width):
            added_ref[first + side] = rows[:, side * LANES : (side + 1) * LANES]

    def place_many(index, carry):
        for part in range(PAIRS):
            place_rows(2 * (PAIRS * index + part), 2)
        return carry

    steps = nodes // (2 * PAIRS)
    lax.fori_loop(0, steps, place_many, 0)
    for first in range(2 * PAIRS * steps, nodes, 2):
        place_rows(first, min(2, nodes - first))


def annulus_step(
    early, late, emit, stride, first_order, win_ref, harmonic_ref, coefficient_ref,
    keycol_ref, below_ref, above_ref, value_ref, previous_ref, force_ref, mass_ref, modes_ref,
    next_ref, reaction_ref, terms_ref, added_ref,
):
    nodes, columns, elements = value_ref.shape
    count = reaction_ref.shape[1]
    shared = below_ref.shape[1]
    react_into(win_ref, harmonic_ref, coefficient_ref, stride, reaction_ref)
    finish(early)
    terms_ref[:, 0:count] = stacked(reaction_ref[...])
    terms_ref[:, count : count + shared] = stacked(below_ref[...])
    terms_ref[:, count + shared : count + 2 * shared] = stacked(above_ref[...])
    place_into(terms_ref, keycol_ref, elements, nodes, added_ref)
    order = first_order + iota((columns, elements), 0)
    finish(late)
    live = order < modes_ref[...]
    for node in range(nodes):
        gain = jnp.where(live, step_scale / mass_ref[node : node + 1, :], 0.0)
        next_ref[node] = (
            2.0 * value_ref[node]
            - previous_ref[node]
            + gain * (force_ref[node] + added_ref[node])
        )
        emit(node)


def middle_kernel(
    stride, box_ref, win_ref, samples_ref, node_ref, harmonic_ref,
    keycol_hbm, below_hbm, above_hbm, value_hbm, previous_hbm, force_hbm, mass_hbm, modes_hbm,
    key_hbm, forward_hbm, backward_hbm, radial_hbm, shear_hbm,
    sample_ref, boxnext_ref, next_hbm, nextforce_hbm, low_hbm, high_hbm,
    keycol_ref, below_ref, above_ref, value_ref, previous_ref, force_ref, mass_ref, modes_ref,
    key_ref, forward_ref, backward_ref, radial_ref, shear_ref,
    next_ref, low_ref, high_ref,
    coefficient_ref, reaction_ref, terms_ref, added_ref, stack_ref, picked_ref,
    done, kept,
):
    moves = transfers(
        [
            (keycol_hbm, keycol_ref), (below_hbm, below_ref), (above_hbm, above_ref),
            (value_hbm, value_ref), (previous_hbm, previous_ref), (force_hbm, force_ref),
            (mass_hbm, mass_ref), (modes_hbm, modes_ref), (key_hbm, key_ref),
            (forward_hbm, forward_ref), (backward_hbm, backward_ref), (radial_hbm, radial_ref),
            (shear_hbm, shear_ref),
        ],
        done,
    )
    saves = transfers(
        [
            (next_ref, next_hbm), (added_ref, nextforce_hbm), (low_ref, low_hbm),
            (high_ref, high_hbm),
        ],
        kept,
    )
    begin(moves)
    columns = value_ref.shape[1]
    first_order = box_ref[0] * columns % MODES
    nodes_step(samples_ref, node_ref, node_ref[3], node_ref[4], boxnext_ref, coefficient_ref)
    annulus_step(
        moves[:3], moves[3:], lambda node: None,
        stride, first_order, win_ref, harmonic_ref, coefficient_ref, keycol_ref,
        below_ref, above_ref, value_ref, previous_ref, force_ref, mass_ref, modes_ref,
        next_ref, reaction_ref, terms_ref, added_ref,
    )
    begin(saves[:1])
    force_into(
        next_ref, forward_ref, backward_ref, radial_ref, shear_ref, first_order, added_ref
    )
    begin(saves[1:2])
    fill_stack(added_ref, stack_ref)
    pick_boundary(stack_ref, key_ref, low_ref, high_ref)
    begin(saves[2:])
    fill_stack(next_ref, stack_ref)
    pick_rows(stack_ref, key_ref, picked_ref)
    sample_into(win_ref, harmonic_ref, picked_ref, stride, sample_ref)
    finish(saves)


def box_kernel(copies, box_ref, samples_ref, node_ref, now_ref, own_ref, coefficient_ref, *scratch):
    boxnext_ref = scratch[0] if scratch else own_ref
    nodes_step(samples_ref, node_ref, now_ref[...], node_ref[3], boxnext_ref, coefficient_ref)
    if scratch:
        for index in range(own_ref.shape[0]):
            own_ref[index : index + 1, :] = boxnext_ref[pl.ds(index * copies + box_ref[0], 1), :]


def last_kernel(
    stride, box_ref, win_ref, coefficient_ref, harmonic_ref,
    keycol_hbm, below_hbm, above_hbm, value_hbm, previous_hbm, force_hbm, mass_hbm, modes_hbm,
    next_hbm,
    keycol_ref, below_ref, above_ref, value_ref, previous_ref, force_ref, mass_ref, modes_ref,
    next_ref, reaction_ref, terms_ref, added_ref, done, kept,
):
    moves = transfers(
        [
            (keycol_hbm, keycol_ref), (below_hbm, below_ref), (above_hbm, above_ref),
            (value_hbm, value_ref), (previous_hbm, previous_ref), (force_hbm, force_ref),
            (mass_hbm, mass_ref), (modes_hbm, modes_ref),
        ],
        done,
    )
    begin(moves)
    first_order = box_ref[0] * value_ref.shape[1] % MODES
    saves = transfers(
        [(next_ref.at[node], next_hbm.at[node]) for node in range(value_ref.shape[0])], kept
    )
    annulus_step(
        moves[:3], moves[3:], lambda node: saves[node].start(),
        stride, first_order, win_ref, harmonic_ref, coefficient_ref, keycol_ref,
        below_ref, above_ref, value_ref, previous_ref, force_ref, mass_ref, modes_ref,
        next_ref, reaction_ref, terms_ref, added_ref,
    )
    finish(saves)


def exchanged(low, high):
    size = lax.axis_size("mer")
    up = [(i, i + 1) for i in range(size - 1)]
    down = [(j, i) for i, j in up]
    return lax.ppermute(high, "mer", up), lax.ppermute(low, "mer", down)


SMEM, VMEM, HBM = pltpu.SMEM, pltpu.VMEM, pltpu.HBM


def call(kernel, ins, outs, scratch=(), copies=(), name=None, limit=40, flops=0):
    arrays = [
        pltpu.with_memory_space_constraint(array, memory) if pinned else array
        for array, memory, pinned in ins
    ]
    return pl.pallas_call(
        kernel,
        out_shape=[
            memory(shape, dtype) if memory else jax.ShapeDtypeStruct(shape, dtype)
            for shape, dtype, memory in outs
        ],
        in_specs=[pl.BlockSpec(memory_space=memory) for _, memory, _ in ins],
        out_specs=[pl.BlockSpec(memory_space=memory or VMEM) for _, _, memory in outs],
        scratch_shapes=[VMEM(shape, dtype) for shape, dtype in scratch]
        + [pltpu.SemaphoreType.DMA((number,)) for number in copies],
        compiler_params=pltpu.CompilerParams(vmem_limit_bytes=limit << 20),
        cost_estimate=pl.CostEstimate(flops=flops, transcendentals=0, bytes_accessed=0)
        if flops
        else None,
        name=name,
    )(*arrays)


def per_device(
    annulus,
    annulus_prev,
    derivative,
    radial_modulus,
    shear_modulus,
    node_mass,
    element_modes,
    upper_rows,
    lower_rows,
    coupling_rows,
    coupling_target,
    box_field,
    box_prev,
    box_angle,
    box_spring,
    box_mass,
    box_weight,
    box_slot,
):
    mer_count = lax.axis_size("mer")
    box_count = lax.axis_size("box")
    blocks = mer_count * box_count
    nodes, columns, elements = annulus.shape
    box_nodes = box_slot.shape[0]
    per = box_nodes // mer_count
    stride = LANES // per
    groups = blocks * per // LANES
    count = coupling_rows.shape[0]
    shared = upper_rows.shape[0]
    depth = count + 2 * shared
    padded_nodes = nodes + nodes % 2
    rows = -(-8 * nodes // 16) * 16
    volume = (nodes, columns, elements)
    grid = (groups, LANES)
    flat = (nodes, elements)
    stack_scratch = ((2 * columns, padded_nodes * elements), bf16)

    def far(value):
        return value, HBM, True

    def near(value):
        return value, VMEM, True

    def landed(value):
        return value, VMEM, False

    def anywhere(value):
        return value, pl.ANY, False

    def scalar(value):
        return value, SMEM, False

    box = scalar(jnp.full((1,), lax.axis_index("box"), i32))

    sent = [
        far(value.reshape(1, box_nodes))
        for value in (box_slot, box_angle, box_spring, box_mass, box_weight, box_field, box_prev)
    ]
    line = ((1, box_nodes), i32)
    messages, part, rank = call(
        functools.partial(group_kernel, mer_count, box_count),
        sent,
        [((blocks, 8, per), f32, None), line + (HBM,), line + (HBM,)],
        [line, line, line, ((8, box_nodes), f32)],
        copies=(9,),
        name="group",
    )
    messages = lax.all_to_all(messages, ("mer", "box"), split_axis=0, concat_axis=0, tiled=True)
    if stride > 1:
        messages = messages.reshape(groups, stride, 8, per).swapaxes(1, 2)
        messages = messages.reshape(groups, 8, LANES)

    field = (volume, f32)
    table = (flat, f32)
    limits = ((1, elements), i32)
    side = ((columns, shared), f32)
    keys = [((1, depth), i32), ((depth, LANES), i32)]
    matrices = [((2 * rows, 8 * nodes), bf16)] * 2
    picked = ((2 * columns, count), bf16)
    counts = ((blocks, LANES), f32)
    kept = [counts, counts, picked] + keys + matrices + [field, side, side]
    (
        window, offset, filled, chosen, key, keycol, forward, backward, force, low, high,
    ) = call(
        functools.partial(start_kernel, elements),
        [
            box,
            far(coupling_target.reshape(1, count)),
            far(coupling_rows.reshape(1, count)),
            far(lower_rows.reshape(1, shared)),
            far(upper_rows.reshape(1, shared)),
            far(derivative),
            far(annulus),
            far(radial_modulus),
            far(shear_modulus),
        ],
        [
            ((1, blocks), i32, None),
        ]
        + [shape + (HBM,) for shape in kept],
        [((1, count), i32)] * 2
        + [((1, shared), i32)] * 2
        + [((nodes, nodes), f32), field, table, table]
        + kept
        + [stack_scratch],
        copies=(8, 10),
        name="start",
        flops=4 * columns * nodes * elements * (count + 2 * shared),
    )
    if stride > 1:
        offset = jnp.repeat(offset[:, 0], per).reshape(groups, LANES)
        filled = jnp.repeat(filled[:, 0], per).reshape(groups, LANES)
    window = scalar(window)
    below, above = exchanged(low, high)

    harmonic, node, sample = call(
        functools.partial(node_kernel, stride),
        [box, window, landed(messages), far(offset), far(filled), far(chosen)],
        [
            ((groups, columns + 8, LANES), f32, VMEM),
            ((5, groups, LANES), f32, VMEM),
            (grid, f32, None),
        ],
        [(grid, f32), (grid, f32), picked, (grid, f32)]
        + [((6, groups, LANES), f32)]
        + [((columns // 8, groups, LANES), f32)] * 2,
        copies=(3,),
        name="nodes",
        flops=4 * columns * groups * LANES * WIDE,
    )
    samples = lax.all_gather(sample, "box")

    modes = element_modes.reshape(1, elements)
    fetched = keys[1:] + [side, side, field, field, field, table, limits]
    step_scratch = [
        ((columns, count), f32),
        ((2 * columns, depth), bf16),
        field,
    ]
    sample, box_now, current, force, low, high = call(
        functools.partial(middle_kernel, stride),
        [
            box, window, landed(samples), near(node), near(harmonic),
            far(keycol), anywhere(below), anywhere(above), far(annulus), far(annulus_prev), far(force),
            far(node_mass), far(modes), far(key), far(forward), far(backward),
            far(radial_modulus), far(shear_modulus),
        ],
        [(grid, f32, None), (grid, f32, VMEM)]
        + [shape + (HBM,) for shape in (field, field, side, side)],
        fetched
        + keys[:1]
        + matrices
        + [table, table, field, side, side]
        + [(grid, f32)]
        + step_scratch
        + [stack_scratch, picked],
        copies=(13, 4),
        name="middle",
        flops=8 * columns * nodes * elements * (count + 2 * shared),
    )
    below, above = exchanged(low, high)
    samples = lax.all_gather(sample, "box")

    direct = stride == 1
    returned, coefficient = call(
        functools.partial(box_kernel, box_count),
        [box, landed(samples), near(node), near(box_now)],
        [((mer_count, per) if direct else grid, f32, None), (grid, f32, VMEM)],
        [(grid, f32)] * direct,
        name="box",
    )
    if not direct:
        returned = lax.dynamic_index_in_dim(
            returned.reshape(mer_count, box_count, per), lax.axis_index("box"), axis=1, keepdims=False
        )
    returned = lax.all_to_all(returned, "mer", split_axis=0, concat_axis=0, tiled=True)
    (current,) = call(
        functools.partial(last_kernel, stride),
        [
            box, window, near(coefficient), near(harmonic), far(keycol),
            anywhere(below), anywhere(above), far(current), far(annulus), far(force), far(node_mass), far(modes),
        ],
        [field + (HBM,)],
        fetched + [field] + step_scratch,
        copies=(8, nodes),
        name="last",
        flops=4 * columns * nodes * elements * (count + 2 * shared),
    )
    current, returned = lax.optimization_barrier((current, returned))
    (box_out,) = call(
        ungroup_kernel,
        [landed(part), landed(rank), landed(returned)],
        [((1, box_nodes), f32, None)],
        name="ungroup",
    )
    return current, box_out.reshape(box_nodes)


def solution(mesh):
    in_specs = (
        P(None, "box", "mer"),
        P(None, "box", "mer"),
        P(),
        P(None, "mer"),
        P(None, "mer"),
        P(None, "mer"),
        P("mer"),
        P("mer"),
        P("mer"),
        P("mer"),
        P("mer", None),
        P(("mer", "box")),
        P(("mer", "box")),
        P(("mer", "box")),
        P(("mer", "box")),
        P(("mer", "box")),
        P(("mer", "box")),
        P(("mer", "box")),
    )
    out_specs = (P(None, "box", "mer"), P(("mer", "box")))
    return jax.shard_map(
        per_device, mesh=mesh, in_specs=in_specs, out_specs=out_specs, check_vma=False
    )
```

```python
import functools

import jax
import jax.numpy as jnp
from jax import lax
from jax.experimental import pallas as pl
from jax.experimental.pallas import tpu as pltpu
from jax.sharding import PartitionSpec as P

MODES = 256
STEPS = 2
LANES = 128
WIDE = 256
BATCH = 16
SAMPLES = 32
PAIRS = 6
CHAINS = 4

step_scale = 0.25
f32 = jnp.float32
bf16 = jnp.bfloat16
i32 = jnp.int32


def iota(shape, dim):
    return lax.broadcasted_iota(i32, shape, dim)


def dot(a, b):
    return lax.dot_general(a, b, (((1,), (0,)), ((), ())), preferred_element_type=f32)


def dot_nt(a, b):
    return lax.dot_general(a, b, (((1,), (1,)), ((), ())), preferred_element_type=f32)


def hot(mask):
    return jnp.where(mask, 1.0, 0.0).astype(bf16)


def split(x):
    high = x.astype(bf16)
    return high, (x - high.astype(f32)).astype(bf16)


def stacked(x):
    high, low = split(x)
    return jnp.concatenate([high, low], axis=0)


def folded(x):
    half = x.shape[0] // 2
    return x[:half] + x[half:]


def thirds(x):
    first = x.astype(bf16).astype(f32)
    second = (x - first).astype(bf16).astype(f32)
    return jnp.concatenate([first, second, x - first - second], axis=0)


def cos_sin(x):
    turns = jnp.floor(x * 0.6366197723675814 + 0.5)
    r = x - turns * 1.5703125 - turns * 4.837512969970703125e-4 - turns * 7.54978995489188216e-8
    z = r * r
    sine = ((-1.9515295891e-4 * z + 8.3321608736e-3) * z - 1.6666654611e-1) * z * r + r
    cosine = ((2.443315711809948e-5 * z - 1.388731625493765e-3) * z + 4.166664568298827e-2) * z * z
    cosine = cosine - 0.5 * z + 1.0
    quarter = turns.astype(i32)
    odd = (quarter & 1) == 1
    cosine, sine = jnp.where(odd, sine, cosine), jnp.where(odd, cosine, sine)
    return (
        jnp.where(((quarter + 1) & 2) == 2, -cosine, cosine),
        jnp.where((quarter & 2) == 2, -sine, sine),
    )


def running(mask):
    rows, width = mask.shape
    below = hot(iota((LANES, LANES), 0) < iota((LANES, LANES), 1))
    total = jnp.zeros((rows, 1), f32)
    counts = []
    for start in range(0, width, LANES):
        block = mask[:, start : start + LANES]
        counts.append(dot(block.astype(bf16), below) + total)
        total = total + jnp.sum(block, axis=1, keepdims=True)
    return jnp.concatenate(counts, axis=1), total


def group_kernel(parts, copies, slot_hbm, *refs):
    fields, refs = refs[:6], refs[6:]
    out_ref, part_hbm, rank_hbm, part_ref, rank_ref, slot_ref, stack_ref, done = refs
    nodes = slot_ref.shape[1]
    per = nodes // parts
    stack_ref[...] = jnp.zeros_like(stack_ref)
    moves = [pltpu.make_async_copy(slot_hbm, slot_ref, done.at[0])]
    for index, field in enumerate(fields):
        moves.append(
            pltpu.make_async_copy(field, stack_ref.at[index + 1 : index + 2, :], done.at[index + 1])
        )
    for move in moves:
        move.start()
    moves[0].wait()
    slot = slot_ref[...].astype(f32)
    place = jnp.floor((slot + 0.5) * (1.0 / parts))
    part = (slot - place * parts).astype(i32)
    rows = max(16, parts)
    mask = jnp.where(iota((rows, nodes), 0) == part, 1.0, 0.0)
    count, _ = running(mask)
    rank = jnp.sum(mask * count, axis=0, keepdims=True).astype(i32)
    part_ref[...] = part
    rank_ref[...] = rank
    kept = [
        pltpu.make_async_copy(part_ref, part_hbm, done.at[7]),
        pltpu.make_async_copy(rank_ref, rank_hbm, done.at[8]),
    ]
    for move in kept:
        move.start()
    for move in moves[1:]:
        move.wait()
    stack_ref[0:1, :] = place
    terms = thirds(stack_ref[...])
    blocks = [jnp.where(part == index, terms, 0.0) for index in range(parts)]
    chosen = hot(iota((per, nodes), 0) == rank)
    moved = dot_nt(jnp.concatenate(blocks, axis=0).astype(bf16), chosen)
    for index in range(parts):
        block = moved[24 * index : 24 * index + 24]
        block = block[0:8] + block[8:16] + block[16:24]
        for copy in range(copies):
            out_ref[index * copies + copy] = block
    for move in kept:
        move.wait()


def ungroup_kernel(part_ref, rank_ref, value_ref, out_ref):
    parts, per = value_ref.shape
    nodes = part_ref.shape[1]
    chosen = hot(iota((per, nodes), 0) == rank_ref[...])
    back = dot(thirds(value_ref[...]).astype(bf16), chosen)
    back = back[0:parts] + back[parts : 2 * parts] + back[2 * parts :]
    mask = iota((parts, nodes), 0) == part_ref[...]
    out_ref[...] = jnp.sum(jnp.where(mask, back, 0.0), axis=0, keepdims=True)


def order_rows(
    elements, target_ref, rows_ref, lower_ref, upper_ref, key_ref, keycol_ref, off_ref, cnt_ref, win_ref
):
    blocks = off_ref.shape[0]
    count = target_ref.shape[1]
    shared = lower_ref.shape[1]
    mask = jnp.where(iota((blocks, count), 0) == target_ref[...], 1.0, 0.0)
    before, total = running(mask)
    totals = jnp.broadcast_to(total, (blocks, LANES))
    offset = dot(hot(iota((blocks, blocks), 1) < iota((blocks, blocks), 0)), totals.astype(bf16))
    off_ref[...] = offset
    cnt_ref[...] = totals
    window = jnp.floor(offset * (1.0 / LANES)) * LANES
    win_ref[...] = jnp.minimum(window, count - WIDE).T[0:1, :].astype(i32)
    place = jnp.sum(mask * (before + offset[:, 0:1]), axis=0, keepdims=True)
    strip = jnp.floor((place + 0.5) * (1.0 / LANES))
    lane = (place - strip * LANES).astype(i32)
    row = rows_ref[...].astype(f32)
    node = jnp.floor((row + 0.5) * (1.0 / elements))
    strips = count // LANES
    chosen = iota((strips, count), 0) == strip.astype(i32)
    terms = jnp.concatenate(
        [jnp.where(chosen, node, 0.0), jnp.where(chosen, row - node * elements, 0.0)], axis=0
    )
    moved = dot_nt(terms.astype(bf16), hot(iota((LANES, count), 0) == lane))
    moved = (moved[:strips] * elements + moved[strips:]).astype(i32)
    for index in range(strips):
        key_ref[:, index * LANES : (index + 1) * LANES] = moved[index : index + 1]
    key_ref[:, count : count + shared] = lower_ref[...]
    key_ref[:, count + shared : count + 2 * shared] = upper_ref[...]
    for start in range(0, count + 2 * shared, LANES):
        block = jnp.broadcast_to(key_ref[:, start : start + LANES].astype(f32), (LANES, LANES))
        keycol_ref[start : start + LANES, :] = block.T.astype(i32)


def fill_stack(value_ref, stack_ref):
    nodes, columns, elements = value_ref.shape
    for node in range(nodes):
        high, low = split(value_ref[node])
        lanes = slice(node * elements, (node + 1) * elements)
        stack_ref[0:columns, lanes] = high
        stack_ref[columns:, lanes] = low
    if stack_ref.shape[1] > nodes * elements:
        tail = slice(nodes * elements, stack_ref.shape[1])
        stack_ref[:, tail] = jnp.zeros_like(stack_ref[:, tail])


def picked(stack_ref, key_ref, start):
    key = key_ref[:, pl.ds(start, WIDE)]
    base = iota((LANES, WIDE), 0)
    chosen = [hot(base == key - row) for row in range(0, stack_ref.shape[1], LANES)]
    return dot(stack_ref[...], jnp.concatenate(chosen, axis=0))


def pick_rows(stack_ref, key_ref, out_ref):
    def body(index, carry):
        for part in range(4):
            start = pl.multiple_of((4 * index + part) * WIDE, WIDE)
            out_ref[:, pl.ds(start, WIDE)] = picked(stack_ref, key_ref, start).astype(bf16)
        return carry

    lax.fori_loop(0, out_ref.shape[1] // (4 * WIDE), body, 0)


def pick_boundary(stack_ref, key_ref, low_ref, high_ref):
    shared = low_ref.shape[1]
    first = key_ref.shape[1] - 2 * shared
    for ref, origin in ((low_ref, first), (high_ref, first + shared)):
        for start in range(0, shared, WIDE):
            ref[:, start : start + WIDE] = folded(picked(stack_ref, key_ref, origin + start))


def spread(derivative_ref, transposed, rows):
    nodes = derivative_ref.shape[0]
    size = 8 * nodes
    left = hot(iota((rows, nodes), 0) // 8 == iota((rows, nodes), 1))
    right = hot(iota((nodes, size), 1) // 8 == iota((nodes, size), 0))
    same = iota((rows, size), 0) % 8 == iota((rows, size), 1) % 8
    parts = []
    for term in split(derivative_ref[...]):
        half = (dot_nt if transposed else dot)(left, term)
        parts.append(jnp.where(same, dot(half.astype(bf16), right), 0.0))
    return jnp.concatenate(parts, axis=0).astype(bf16)


def force_into(
    value_ref, previous_ref, forward, backward, radial_ref, shear_ref, mass_ref, modes_ref,
    first_order, force_ref, drift_ref,
):
    nodes, columns, elements = value_ref.shape
    size = 8 * nodes
    rows = forward.shape[0] // 2
    radial = jnp.broadcast_to(radial_ref[...][:, None, :], (nodes, 8, elements)).reshape(
        size, elements
    )
    radial = jnp.concatenate([radial, radial], axis=1)
    shear = jnp.broadcast_to(shear_ref[...][:, None, :], (nodes, 8, elements))
    scale = jnp.broadcast_to((step_scale / mass_ref[...])[:, None, :], (nodes, 8, elements))

    def applied(matrix, x):
        high, low = split(x)
        both = dot(matrix[...], high)
        return both[:size] + both[rows : rows + size] + dot(matrix[0:rows, :], low)[:size]

    def body(index, carry):
        first = pl.multiple_of(index * 16 * CHAINS, 16 * CHAINS)
        starts = [first + 16 * chain for chain in range(CHAINS)]
        halves = [
            [value_ref[:, pl.ds(start, 8), :], value_ref[:, pl.ds(start + 8, 8), :]]
            for start in starts
        ]
        fields = [
            jnp.concatenate([half.reshape(size, elements) for half in pair], axis=1)
            for pair in halves
        ]
        fluxes = [radial * applied(forward, x) for x in fields]
        backs = [applied(backward, flux) for flux in fluxes]
        for start, pair, back in zip(starts, halves, backs):
            for side, half in enumerate(pair):
                part = pl.ds(start + 8 * side, 8)
                order = first_order + start + 8 * side + iota((8, elements), 0)
                wave = (2.0 * order.astype(f32) / MODES) ** 2
                block = back[:, side * elements : (side + 1) * elements]
                force = -block.reshape(nodes, 8, elements) - shear * wave[None] * half
                gain = jnp.where((order < modes_ref[...])[None], scale, 0.0)
                force_ref[:, part, :] = force
                drift_ref[:, part, :] = 2.0 * half - previous_ref[:, part, :] + gain * force
        return carry

    lax.fori_loop(0, columns // (16 * CHAINS), body, 0)


def transfers(pairs, done):
    return [
        pltpu.make_async_copy(source, target, done.at[index])
        for index, (source, target) in enumerate(pairs)
    ]


def begin(moves):
    for move in moves:
        move.start()


def finish(moves):
    for move in moves:
        move.wait()


def start_kernel(
    elements, box_ref, target_hbm, rows_hbm, lower_hbm, upper_hbm, derivative_hbm,
    value_hbm, radial_hbm, shear_hbm, mass_hbm, modes_hbm, previous_hbm,
    win_ref, off_hbm, cnt_hbm, picked_hbm, key_hbm, keycol_hbm, forward_hbm, backward_hbm, drift_hbm, low_hbm, high_hbm,
    target_ref, rows_ref, lower_ref, upper_ref, derivative_ref, value_ref, radial_ref, shear_ref,
    mass_ref, modes_ref, previous_ref,
    off_ref, cnt_ref, picked_ref, key_ref, keycol_ref, forward_ref, backward_ref, drift_ref, low_ref,
    high_ref, force_ref, stack_ref, done, kept,
):
    moves = transfers(
        [
            (target_hbm, target_ref), (rows_hbm, rows_ref), (lower_hbm, lower_ref),
            (upper_hbm, upper_ref), (derivative_hbm, derivative_ref), (value_hbm, value_ref),
            (radial_hbm, radial_ref), (shear_hbm, shear_ref), (mass_hbm, mass_ref),
            (modes_hbm, modes_ref), (previous_hbm, previous_ref),
        ],
        done,
    )
    saves = transfers(
        [
            (off_ref, off_hbm), (cnt_ref, cnt_hbm), (picked_ref, picked_hbm),
            (key_ref, key_hbm), (keycol_ref, keycol_hbm), (forward_ref, forward_hbm),
            (backward_ref, backward_hbm), (drift_ref, drift_hbm), (low_ref, low_hbm),
            (high_ref, high_hbm),
        ],
        kept,
    )
    begin(moves)
    finish(moves[:5])
    order_rows(
        elements, target_ref, rows_ref, lower_ref, upper_ref, key_ref, keycol_ref, off_ref,
        cnt_ref, win_ref,
    )
    columns = value_ref.shape[1]
    rows = forward_ref.shape[0] // 2
    forward_ref[...] = spread(derivative_ref, False, rows)
    backward_ref[...] = spread(derivative_ref, True, rows)
    begin(saves[:2] + saves[3:7])
    finish(moves[5:6])
    fill_stack(value_ref, stack_ref)
    pick_rows(stack_ref, key_ref, picked_ref)
    begin(saves[2:3])
    finish(moves[6:])
    force_into(
        value_ref, previous_ref, forward_ref, backward_ref, radial_ref, shear_ref, mass_ref,
        modes_ref, box_ref[0] * columns % MODES, force_ref, drift_ref,
    )
    begin(saves[7:8])
    fill_stack(force_ref, stack_ref)
    pick_boundary(stack_ref, key_ref, low_ref, high_ref)
    begin(saves[8:])
    finish(saves)


def window_hot(win_ref, harmonic_ref, group, stride):
    window = pl.multiple_of(win_ref[0, group * stride], LANES)
    columns = harmonic_ref.shape[1] - 8
    place = harmonic_ref[group, columns : columns + 1, :].astype(i32)
    return window, hot(iota((WIDE, LANES), 0) + window == place)


def sample_into(win_ref, harmonic_ref, picked_ref, stride, sample_ref):
    columns = harmonic_ref.shape[1] - 8

    def body(index, carry):
        for group in [SAMPLES * index + part for part in range(SAMPLES)]:
            window, chosen = window_hot(win_ref, harmonic_ref, group, stride)
            rows = folded(dot(picked_ref[:, pl.ds(window, WIDE)], chosen))
            sample_ref[pl.ds(group, 1), :] = jnp.sum(
                rows * harmonic_ref[group, 0:columns, :], axis=0, keepdims=True
            )
        return carry

    lax.fori_loop(0, sample_ref.shape[0] // SAMPLES, body, 0)


def times(x, y):
    return x[0] * y[0] - x[1] * y[1], x[0] * y[1] + x[1] * y[0]


def node_kernel(
    stride, box_ref, win_ref, message_ref, off_hbm, cnt_hbm, picked_hbm,
    harmonic_ref, node_ref, sample_ref,
    off_ref, cnt_ref, picked_ref, place_ref, near_ref, far_re, far_im, done,
):
    moves = transfers(
        [(off_hbm, off_ref), (cnt_hbm, cnt_ref), (picked_hbm, picked_ref)], done
    )
    begin(moves)
    groups, columns = harmonic_ref.shape[0], harmonic_ref.shape[1] - 8
    place = message_ref[:, 0, :]
    angle = message_ref[:, 1, :]
    for index in range(5):
        node_ref[index] = message_ref[:, 2 + index, :]
    for bit in range(3):
        re, im = cos_sin(float(1 << bit) * angle)
        near_ref[2 * bit] = re
        near_ref[2 * bit + 1] = im
    first = box_ref[0] * columns
    base_re, base_im = cos_sin((first % MODES).astype(f32) * angle)
    sine = first >= MODES
    far = [
        (jnp.where(sine, base_im, base_re), jnp.where(sine, -base_re, base_im))
    ] + [None] * (columns // 8 - 1)
    bit = 1
    while bit < columns // 8:
        factor = cos_sin(float(8 * bit) * angle)
        for low in range(min(bit, columns // 8 - bit)):
            far[bit + low] = times(factor, far[low])
        bit *= 2
    for index, (re, im) in enumerate(far):
        far_re[index] = re
        far_im[index] = im
    finish(moves[:2])
    place_ref[...] = jnp.where(place < cnt_ref[...], off_ref[...] + place, -1.0)
    order = iota((8, LANES), 0)

    def body(index, carry):
        for group in [4 * index + part for part in range(4)]:
            row = pl.ds(group, 1)
            powers = [
                (
                    jnp.where((order >> bit) & 1 == 1, near_ref[2 * bit, row, :], 1.0),
                    jnp.where((order >> bit) & 1 == 1, near_ref[2 * bit + 1, row, :], 0.0),
                )
                for bit in range(3)
            ]
            re, im = times(times(powers[0], powers[1]), powers[2])
            for step in range(columns // 8):
                harmonic_ref[group, 8 * step : 8 * step + 8, :] = (
                    far_re[step, row, :] * re - far_im[step, row, :] * im
                )
            harmonic_ref[group, columns : columns + 8, :] = jnp.broadcast_to(
                place_ref[row, :], (8, LANES)
            )
        return carry

    lax.fori_loop(0, groups // 4, body, 0)
    finish(moves[2:])
    sample_into(win_ref, harmonic_ref, picked_ref, stride, sample_ref)


def nodes_step(samples_ref, node_ref, now, before, next_ref, coefficient_ref):
    sample = samples_ref[0]
    for index in range(1, samples_ref.shape[0]):
        sample = sample + samples_ref[index]
    pull = node_ref[0] * (sample - now)
    next_ref[...] = 2.0 * now - before + step_scale * pull / node_ref[1]
    coefficient_ref[...] = -node_ref[2] * pull


def react_into(win_ref, harmonic_ref, coefficient_ref, stride, reaction_ref):
    reaction_ref[...] = jnp.zeros_like(reaction_ref)
    columns = reaction_ref.shape[0]

    def react(index, carry):
        found = []
        for group in [BATCH * index + part for part in range(BATCH)]:
            window, chosen = window_hot(win_ref, harmonic_ref, group, stride)
            weighted = harmonic_ref[group, 0:columns, :] * coefficient_ref[pl.ds(group, 1), :]
            found.append((window, folded(dot_nt(stacked(weighted), chosen))))
        for window, rows in found:
            reaction_ref[:, pl.ds(window, WIDE)] = reaction_ref[:, pl.ds(window, WIDE)] + rows
        return carry

    lax.fori_loop(0, harmonic_ref.shape[0] // BATCH, react, 0)


def place_into(terms_ref, keycol_ref, elements, nodes, emit, flush):
    depth = terms_ref.shape[1]
    lane = iota((LANES, LANES), 1)

    def place_rows(first, width):
        sides = []
        for side in range(width):
            base = lane + (first + side) * elements
            chosen = [
                hot(keycol_ref[row : row + LANES, :] == base) for row in range(0, depth, LANES)
            ]
            sides.append(jnp.concatenate(chosen, axis=0))
        rows = folded(dot(terms_ref[...], jnp.concatenate(sides, axis=1)))
        for side in range(width):
            emit(first + side, rows[:, side * LANES : (side + 1) * LANES])

    def place_many(index, carry):
        for part in range(PAIRS):
            place_rows(2 * (PAIRS * index + part), 2)
        flush(2 * PAIRS * index, 2 * PAIRS, index)
        return carry

    steps = nodes // (2 * PAIRS)
    lax.fori_loop(0, steps, place_many, 0)
    for first in range(2 * PAIRS * steps, nodes, 2):
        place_rows(first, min(2, nodes - first))
    if nodes > 2 * PAIRS * steps:
        flush(2 * PAIRS * steps, nodes - 2 * PAIRS * steps, steps)


def annulus_step(
    early, late, after, flush, stride, first_order, win_ref, harmonic_ref, coefficient_ref,
    keycol_ref, below_ref, above_ref, drift_ref, mass_ref, modes_ref,
    next_ref, reaction_ref, terms_ref,
):
    nodes, columns, elements = drift_ref.shape
    count = reaction_ref.shape[1]
    shared = below_ref.shape[1]
    react_into(win_ref, harmonic_ref, coefficient_ref, stride, reaction_ref)
    finish(early)
    terms_ref[:, 0:count] = stacked(reaction_ref[...])
    terms_ref[:, count : count + shared] = stacked(below_ref[...])
    terms_ref[:, count + shared : count + 2 * shared] = stacked(above_ref[...])
    finish(late)
    live = first_order + iota((columns, elements), 0) < modes_ref[...]

    def emit(node, added):
        gain = jnp.where(live, step_scale / mass_ref[pl.ds(node, 1), :], 0.0)
        value = drift_ref[node] + gain * added
        next_ref[node] = value
        after(node, value)

    place_into(terms_ref, keycol_ref, elements, nodes, emit, flush)


def middle_kernel(
    stride, box_ref, win_ref, samples_ref, node_ref, harmonic_ref,
    keycol_hbm, below_hbm, above_hbm, drift_hbm, mass_hbm, modes_hbm,
    value_hbm, key_hbm, forward_hbm, backward_hbm, radial_hbm, shear_hbm,
    sample_ref, boxnext_ref, nextdrift_hbm, low_hbm, high_hbm,
    keycol_ref, below_ref, above_ref, drift_ref, mass_ref, modes_ref,
    value_ref, key_ref, forward_ref, backward_ref, radial_ref, shear_ref,
    next_ref, low_ref, high_ref,
    coefficient_ref, reaction_ref, terms_ref, force_ref, stack_ref, picked_ref,
    done, kept,
):
    moves = transfers(
        [
            (keycol_hbm, keycol_ref), (below_hbm, below_ref), (above_hbm, above_ref),
            (drift_hbm, drift_ref), (mass_hbm, mass_ref), (modes_hbm, modes_ref),
            (value_hbm, value_ref), (key_hbm, key_ref),
            (forward_hbm, forward_ref), (backward_hbm, backward_ref), (radial_hbm, radial_ref),
            (shear_hbm, shear_ref),
        ],
        done,
    )
    saves = transfers(
        [
            (drift_ref, nextdrift_hbm), (low_ref, low_hbm), (high_ref, high_hbm),
        ],
        kept,
    )
    begin(moves)
    columns = value_ref.shape[1]
    first_order = box_ref[0] * columns % MODES
    nodes_step(samples_ref, node_ref, node_ref[3], node_ref[4], boxnext_ref, coefficient_ref)
    elements = value_ref.shape[2]
    if stack_ref.shape[1] > value_ref.shape[0] * elements:
        tail = slice(value_ref.shape[0] * elements, stack_ref.shape[1])
        stack_ref[:, tail] = jnp.zeros_like(stack_ref[:, tail])

    def after(node, value):
        lanes = pl.ds(pl.multiple_of(node * elements, elements), elements)
        high, low = split(value)
        stack_ref[0:columns, lanes] = high
        stack_ref[columns:, lanes] = low

    annulus_step(
        moves[:3], moves[3:6], after, lambda first, size, index: None,
        stride, first_order, win_ref, harmonic_ref, coefficient_ref, keycol_ref,
        below_ref, above_ref, drift_ref, mass_ref, modes_ref,
        next_ref, reaction_ref, terms_ref,
    )
    finish(moves[6:])
    pick_rows(stack_ref, key_ref, picked_ref)
    force_into(
        next_ref, value_ref, forward_ref, backward_ref, radial_ref, shear_ref, mass_ref,
        modes_ref, first_order, force_ref, drift_ref,
    )
    begin(saves[:1])
    fill_stack(force_ref, stack_ref)
    pick_boundary(stack_ref, key_ref, low_ref, high_ref)
    begin(saves[1:])
    sample_into(win_ref, harmonic_ref, picked_ref, stride, sample_ref)
    finish(saves)


def box_kernel(copies, box_ref, samples_ref, node_ref, now_ref, own_ref, coefficient_ref, *scratch):
    boxnext_ref = scratch[0] if scratch else own_ref
    nodes_step(samples_ref, node_ref, now_ref[...], node_ref[3], boxnext_ref, coefficient_ref)
    if scratch:
        for index in range(own_ref.shape[0]):
            own_ref[index : index + 1, :] = boxnext_ref[pl.ds(index * copies + box_ref[0], 1), :]


def last_kernel(
    stride, box_ref, win_ref, coefficient_ref, harmonic_ref,
    keycol_hbm, below_hbm, above_hbm, drift_hbm, mass_hbm, modes_hbm,
    next_hbm,
    keycol_ref, below_ref, above_ref, drift_ref, mass_ref, modes_ref,
    next_ref, reaction_ref, terms_ref, done, kept,
):
    moves = transfers(
        [
            (keycol_hbm, keycol_ref), (below_hbm, below_ref), (above_hbm, above_ref),
            (drift_hbm, drift_ref), (mass_hbm, mass_ref), (modes_hbm, modes_ref),
        ],
        done,
    )
    begin(moves)
    first_order = box_ref[0] * drift_ref.shape[1] % MODES

    def save(first, size, index):
        part = pl.ds(first, size)
        return pltpu.make_async_copy(next_ref.at[part], next_hbm.at[part], kept.at[index])

    annulus_step(
        moves[:3], moves[3:], lambda node, value: None,
        lambda first, size, index: save(first, size, index).start(),
        stride, first_order, win_ref, harmonic_ref, coefficient_ref, keycol_ref,
        below_ref, above_ref, drift_ref, mass_ref, modes_ref,
        next_ref, reaction_ref, terms_ref,
    )
    nodes = drift_ref.shape[0]
    steps = -(-nodes // (2 * PAIRS))
    finish(
        [
            save(2 * PAIRS * index, min(2 * PAIRS, nodes - 2 * PAIRS * index), index)
            for index in range(steps)
        ]
    )


def exchanged(low, high):
    size = lax.axis_size("mer")
    up = [(i, i + 1) for i in range(size - 1)]
    down = [(j, i) for i, j in up]
    return lax.ppermute(high, "mer", up), lax.ppermute(low, "mer", down)


SMEM, VMEM, HBM = pltpu.SMEM, pltpu.VMEM, pltpu.HBM


def call(kernel, ins, outs, scratch=(), copies=(), name=None, limit=40, flops=0):
    arrays = [
        pltpu.with_memory_space_constraint(array, memory) if pinned else array
        for array, memory, pinned in ins
    ]
    return pl.pallas_call(
        kernel,
        out_shape=[
            memory(shape, dtype) if memory else jax.ShapeDtypeStruct(shape, dtype)
            for shape, dtype, memory in outs
        ],
        in_specs=[pl.BlockSpec(memory_space=memory) for _, memory, _ in ins],
        out_specs=[pl.BlockSpec(memory_space=memory or VMEM) for _, _, memory in outs],
        scratch_shapes=[VMEM(shape, dtype) for shape, dtype in scratch]
        + [pltpu.SemaphoreType.DMA((number,)) for number in copies],
        compiler_params=pltpu.CompilerParams(vmem_limit_bytes=limit << 20),
        cost_estimate=pl.CostEstimate(flops=flops, transcendentals=0, bytes_accessed=0)
        if flops
        else None,
        name=name,
    )(*arrays)


def per_device(
    annulus,
    annulus_prev,
    derivative,
    radial_modulus,
    shear_modulus,
    node_mass,
    element_modes,
    upper_rows,
    lower_rows,
    coupling_rows,
    coupling_target,
    box_field,
    box_prev,
    box_angle,
    box_spring,
    box_mass,
    box_weight,
    box_slot,
):
    mer_count = lax.axis_size("mer")
    box_count = lax.axis_size("box")
    blocks = mer_count * box_count
    nodes, columns, elements = annulus.shape
    box_nodes = box_slot.shape[0]
    per = box_nodes // mer_count
    stride = LANES // per
    groups = blocks * per // LANES
    count = coupling_rows.shape[0]
    shared = upper_rows.shape[0]
    depth = count + 2 * shared
    padded_nodes = nodes + nodes % 2
    rows = -(-8 * nodes // 16) * 16
    volume = (nodes, columns, elements)
    grid = (groups, LANES)
    flat = (nodes, elements)
    stack_scratch = ((2 * columns, padded_nodes * elements), bf16)

    def far(value):
        return value, HBM, True

    def near(value):
        return value, VMEM, True

    def landed(value):
        return value, VMEM, False

    def anywhere(value):
        return value, pl.ANY, False

    def scalar(value):
        return value, SMEM, False

    box = scalar(jnp.full((1,), lax.axis_index("box"), i32))

    sent = [
        far(value.reshape(1, box_nodes))
        for value in (box_slot, box_angle, box_spring, box_mass, box_weight, box_field, box_prev)
    ]
    line = ((1, box_nodes), i32)
    messages, part, rank = call(
        functools.partial(group_kernel, mer_count, box_count),
        sent,
        [((blocks, 8, per), f32, VMEM), line + (HBM,), line + (HBM,)],
        [line, line, line, ((8, box_nodes), f32)],
        copies=(9,),
        name="group",
    )
    messages = lax.all_to_all(messages, ("mer", "box"), split_axis=0, concat_axis=0, tiled=True)
    if stride > 1:
        messages = messages.reshape(groups, stride, 8, per).swapaxes(1, 2)
        messages = messages.reshape(groups, 8, LANES)

    field = (volume, f32)
    table = (flat, f32)
    limits = ((1, elements), i32)
    modes = element_modes.reshape(1, elements)
    side = ((columns, shared), f32)
    keys = [((1, depth), i32), ((depth, LANES), i32)]
    matrices = [((2 * rows, 8 * nodes), bf16)] * 2
    picked = ((2 * columns, count), bf16)
    counts = ((blocks, LANES), f32)
    kept = [counts, counts, picked] + keys + matrices + [field, side, side]
    (
        window, offset, filled, chosen, key, keycol, forward, backward, drift, low, high,
    ) = call(
        functools.partial(start_kernel, elements),
        [
            box,
            far(coupling_target.reshape(1, count)),
            far(coupling_rows.reshape(1, count)),
            far(lower_rows.reshape(1, shared)),
            far(upper_rows.reshape(1, shared)),
            far(derivative),
            far(annulus),
            far(radial_modulus),
            far(shear_modulus),
            far(node_mass),
            far(modes),
            far(annulus_prev),
        ],
        [
            ((1, blocks), i32, None),
        ]
        + [shape + (HBM,) for shape in kept],
        [((1, count), i32)] * 2
        + [((1, shared), i32)] * 2
        + [((nodes, nodes), f32), field, table, table, table, limits, field]
        + kept
        + [field, stack_scratch],
        copies=(11, 10),
        name="start",
        flops=4 * columns * nodes * elements * (count + 2 * shared),
    )
    if stride > 1:
        offset = jnp.repeat(offset[:, 0], per).reshape(groups, LANES)
        filled = jnp.repeat(filled[:, 0], per).reshape(groups, LANES)
    window = scalar(window)
    below, above = exchanged(low, high)

    harmonic, node, sample = call(
        functools.partial(node_kernel, stride),
        [box, window, landed(messages), far(offset), far(filled), far(chosen)],
        [
            ((groups, columns + 8, LANES), f32, VMEM),
            ((5, groups, LANES), f32, VMEM),
            (grid, f32, None),
        ],
        [(grid, f32), (grid, f32), picked, (grid, f32)]
        + [((6, groups, LANES), f32)]
        + [((columns // 8, groups, LANES), f32)] * 2,
        copies=(3,),
        name="nodes",
        flops=4 * columns * groups * LANES * WIDE,
    )
    samples = lax.all_gather(sample, "box")

    fetched = keys[1:] + [side, side, field, table, limits]
    step_scratch = [
        ((columns, count), f32),
        ((2 * columns, depth), bf16),
    ]
    sample, box_now, drift, low, high = call(
        functools.partial(middle_kernel, stride),
        [
            box, window, landed(samples), near(node), near(harmonic),
            far(keycol), anywhere(below), anywhere(above), far(drift), far(node_mass), far(modes),
            far(annulus), far(key), far(forward), far(backward), far(radial_modulus),
            far(shear_modulus),
        ],
        [(grid, f32, None), (grid, f32, VMEM)]
        + [shape + (HBM,) for shape in (field, side, side)],
        fetched
        + [field]
        + keys[:1]
        + matrices
        + [table, table, field, side, side]
        + [(grid, f32)]
        + step_scratch
        + [field, stack_scratch, picked],
        copies=(12, 3),
        name="middle",
        flops=8 * columns * nodes * elements * (count + 2 * shared),
    )
    below, above = exchanged(low, high)
    samples = lax.all_gather(sample, "box")

    direct = stride == 1
    returned, coefficient = call(
        functools.partial(box_kernel, box_count),
        [box, landed(samples), near(node), near(box_now)],
        [((mer_count, per) if direct else grid, f32, VMEM), (grid, f32, VMEM)],
        [(grid, f32)] * direct,
        name="box",
    )
    if not direct:
        returned = lax.dynamic_index_in_dim(
            returned.reshape(mer_count, box_count, per), lax.axis_index("box"), axis=1, keepdims=False
        )
    returned = lax.all_to_all(returned, "mer", split_axis=0, concat_axis=0, tiled=True)
    (current,) = call(
        functools.partial(last_kernel, stride),
        [
            box, window, near(coefficient), near(harmonic), far(keycol), anywhere(below),
            anywhere(above), far(drift), far(node_mass), far(modes),
        ],
        [field + (HBM,)],
        fetched + [field] + step_scratch,
        copies=(6, -(-nodes // (2 * PAIRS))),
        name="last",
        flops=4 * columns * nodes * elements * (count + 2 * shared),
    )
    current, returned = lax.optimization_barrier((current, returned))
    (box_out,) = call(
        ungroup_kernel,
        [landed(part), landed(rank), landed(returned)],
        [((1, box_nodes), f32, None)],
        name="ungroup",
    )
    return current, box_out.reshape(box_nodes)


def solution(mesh):
    in_specs = (
        P(None, "box", "mer"),
        P(None, "box", "mer"),
        P(),
        P(None, "mer"),
        P(None, "mer"),
        P(None, "mer"),
        P("mer"),
        P("mer"),
        P("mer"),
        P("mer"),
        P("mer", None),
        P(("mer", "box")),
        P(("mer", "box")),
        P(("mer", "box")),
        P(("mer", "box")),
        P(("mer", "box")),
        P(("mer", "box")),
        P(("mer", "box")),
    )
    out_specs = (P(None, "box", "mer"), P(("mer", "box")))
    return jax.shard_map(
        per_device, mesh=mesh, in_specs=in_specs, out_specs=out_specs, check_vma=False
    )
```

```python
import functools

import jax
import jax.numpy as jnp
from jax import lax
from jax.experimental import pallas as pl
from jax.experimental.pallas import tpu as pltpu
from jax.sharding import PartitionSpec as P

MODES = 256
STEPS = 2
LANES = 128
WIDE = 256
BATCH = 16
SAMPLES = 32
PAIRS = 6
CHAINS = 4

step_scale = 0.25
f32 = jnp.float32
bf16 = jnp.bfloat16
i32 = jnp.int32


def iota(shape, dim):
    return lax.broadcasted_iota(i32, shape, dim)


def dot(a, b):
    return lax.dot_general(a, b, (((1,), (0,)), ((), ())), preferred_element_type=f32)


def dot_nt(a, b):
    return lax.dot_general(a, b, (((1,), (1,)), ((), ())), preferred_element_type=f32)


def hot(mask):
    return jnp.where(mask, 1.0, 0.0).astype(bf16)


def split(x):
    high = x.astype(bf16)
    return high, (x - high.astype(f32)).astype(bf16)


def stacked(x):
    high, low = split(x)
    return jnp.concatenate([high, low], axis=0)


def folded(x):
    half = x.shape[0] // 2
    return x[:half] + x[half:]


def thirds(x):
    first = x.astype(bf16).astype(f32)
    second = (x - first).astype(bf16).astype(f32)
    return jnp.concatenate([first, second, x - first - second], axis=0)


def cos_sin(x):
    turns = jnp.floor(x * 0.6366197723675814 + 0.5)
    r = x - turns * 1.5703125 - turns * 4.837512969970703125e-4 - turns * 7.54978995489188216e-8
    z = r * r
    sine = ((-1.9515295891e-4 * z + 8.3321608736e-3) * z - 1.6666654611e-1) * z * r + r
    cosine = ((2.443315711809948e-5 * z - 1.388731625493765e-3) * z + 4.166664568298827e-2) * z * z
    cosine = cosine - 0.5 * z + 1.0
    quarter = turns.astype(i32)
    odd = (quarter & 1) == 1
    cosine, sine = jnp.where(odd, sine, cosine), jnp.where(odd, cosine, sine)
    return (
        jnp.where(((quarter + 1) & 2) == 2, -cosine, cosine),
        jnp.where((quarter & 2) == 2, -sine, sine),
    )


def running(mask):
    rows, width = mask.shape
    below = hot(iota((LANES, LANES), 0) < iota((LANES, LANES), 1))
    total = jnp.zeros((rows, 1), f32)
    counts = []
    for start in range(0, width, LANES):
        block = mask[:, start : start + LANES]
        counts.append(dot(block.astype(bf16), below) + total)
        total = total + jnp.sum(block, axis=1, keepdims=True)
    return jnp.concatenate(counts, axis=1), total


def group_kernel(parts, copies, slot_hbm, *refs):
    fields, refs = refs[:6], refs[6:]
    out_ref, part_hbm, rank_hbm, part_ref, rank_ref, slot_ref, stack_ref, done = refs
    nodes = slot_ref.shape[1]
    per = nodes // parts
    stack_ref[...] = jnp.zeros_like(stack_ref)
    moves = [pltpu.make_async_copy(slot_hbm, slot_ref, done.at[0])]
    for index, field in enumerate(fields):
        moves.append(
            pltpu.make_async_copy(field, stack_ref.at[index + 1 : index + 2, :], done.at[index + 1])
        )
    for move in moves:
        move.start()
    moves[0].wait()
    slot = slot_ref[...].astype(f32)
    place = jnp.floor((slot + 0.5) * (1.0 / parts))
    part = (slot - place * parts).astype(i32)
    rows = max(16, parts)
    mask = jnp.where(iota((rows, nodes), 0) == part, 1.0, 0.0)
    count, _ = running(mask)
    rank = jnp.sum(mask * count, axis=0, keepdims=True).astype(i32)
    part_ref[...] = part
    rank_ref[...] = rank
    kept = [
        pltpu.make_async_copy(part_ref, part_hbm, done.at[7]),
        pltpu.make_async_copy(rank_ref, rank_hbm, done.at[8]),
    ]
    for move in kept:
        move.start()
    for move in moves[1:]:
        move.wait()
    stack_ref[0:1, :] = place
    terms = thirds(stack_ref[...])
    blocks = [jnp.where(part == index, terms, 0.0) for index in range(parts)]
    chosen = hot(iota((per, nodes), 0) == rank)
    moved = dot_nt(jnp.concatenate(blocks, axis=0).astype(bf16), chosen)
    for index in range(parts):
        block = moved[24 * index : 24 * index + 24]
        block = block[0:8] + block[8:16] + block[16:24]
        for copy in range(copies):
            out_ref[index * copies + copy] = block
    for move in kept:
        move.wait()


def ungroup_kernel(part_ref, rank_ref, value_ref, out_ref):
    parts, per = value_ref.shape
    nodes = part_ref.shape[1]
    chosen = hot(iota((per, nodes), 0) == rank_ref[...])
    back = dot(thirds(value_ref[...]).astype(bf16), chosen)
    back = back[0:parts] + back[parts : 2 * parts] + back[2 * parts :]
    mask = iota((parts, nodes), 0) == part_ref[...]
    out_ref[...] = jnp.sum(jnp.where(mask, back, 0.0), axis=0, keepdims=True)


def order_rows(
    elements, target_ref, rows_ref, lower_ref, upper_ref, key_ref, keycol_ref, off_ref, cnt_ref, win_ref
):
    blocks = off_ref.shape[0]
    count = target_ref.shape[1]
    shared = lower_ref.shape[1]
    mask = jnp.where(iota((blocks, count), 0) == target_ref[...], 1.0, 0.0)
    before, total = running(mask)
    totals = jnp.broadcast_to(total, (blocks, LANES))
    offset = dot(hot(iota((blocks, blocks), 1) < iota((blocks, blocks), 0)), totals.astype(bf16))
    off_ref[...] = offset
    cnt_ref[...] = totals
    window = jnp.floor(offset * (1.0 / LANES)) * LANES
    win_ref[...] = jnp.minimum(window, count - WIDE).T[0:1, :].astype(i32)
    place = jnp.sum(mask * (before + offset[:, 0:1]), axis=0, keepdims=True)
    strip = jnp.floor((place + 0.5) * (1.0 / LANES))
    lane = (place - strip * LANES).astype(i32)
    row = rows_ref[...].astype(f32)
    node = jnp.floor((row + 0.5) * (1.0 / elements))
    strips = count // LANES
    chosen = iota((strips, count), 0) == strip.astype(i32)
    terms = jnp.concatenate(
        [jnp.where(chosen, node, 0.0), jnp.where(chosen, row - node * elements, 0.0)], axis=0
    )
    moved = dot_nt(terms.astype(bf16), hot(iota((LANES, count), 0) == lane))
    moved = (moved[:strips] * elements + moved[strips:]).astype(i32)
    for index in range(strips):
        key_ref[:, index * LANES : (index + 1) * LANES] = moved[index : index + 1]
    key_ref[:, count : count + shared] = lower_ref[...]
    key_ref[:, count + shared : count + 2 * shared] = upper_ref[...]
    for start in range(0, count + 2 * shared, LANES):
        block = jnp.broadcast_to(key_ref[:, start : start + LANES].astype(f32), (LANES, LANES))
        keycol_ref[start : start + LANES, :] = block.T.astype(i32)


def fill_stack(value_ref, stack_ref):
    nodes, columns, elements = value_ref.shape
    for node in range(nodes):
        high, low = split(value_ref[node])
        lanes = slice(node * elements, (node + 1) * elements)
        stack_ref[0:columns, lanes] = high
        stack_ref[columns:, lanes] = low
    if stack_ref.shape[1] > nodes * elements:
        tail = slice(nodes * elements, stack_ref.shape[1])
        stack_ref[:, tail] = jnp.zeros_like(stack_ref[:, tail])


def picked(stack_ref, key_ref, start):
    key = key_ref[:, pl.ds(start, WIDE)]
    base = iota((LANES, WIDE), 0)
    chosen = [hot(base == key - row) for row in range(0, stack_ref.shape[1], LANES)]
    return dot(stack_ref[...], jnp.concatenate(chosen, axis=0))


def pick_rows(stack_ref, key_ref, out_ref):
    def body(index, carry):
        for part in range(8):
            start = pl.multiple_of((8 * index + part) * WIDE, WIDE)
            out_ref[:, pl.ds(start, WIDE)] = picked(stack_ref, key_ref, start).astype(bf16)
        return carry

    lax.fori_loop(0, out_ref.shape[1] // (8 * WIDE), body, 0)


def pick_boundary(stack_ref, key_ref, low_ref, high_ref, saves):
    shared = low_ref.shape[1]
    first = key_ref.shape[1] - 2 * shared
    for ref, origin, save in ((low_ref, first, saves[0]), (high_ref, first + shared, saves[1])):
        for start in range(0, shared, WIDE):
            ref[:, start : start + WIDE] = folded(picked(stack_ref, key_ref, origin + start))
        save.start()


def spread(derivative_ref, transposed, rows):
    nodes = derivative_ref.shape[0]
    size = 8 * nodes
    left = hot(iota((rows, nodes), 0) // 8 == iota((rows, nodes), 1))
    right = hot(iota((nodes, size), 1) // 8 == iota((nodes, size), 0))
    same = iota((rows, size), 0) % 8 == iota((rows, size), 1) % 8
    parts = []
    for term in split(derivative_ref[...]):
        half = (dot_nt if transposed else dot)(left, term)
        parts.append(jnp.where(same, dot(half.astype(bf16), right), 0.0))
    return jnp.concatenate(parts, axis=0).astype(bf16)


def force_into(
    value_ref, previous_ref, forward, backward, radial_ref, shear_ref, mass_ref, modes_ref,
    first_order, force_ref, drift_ref,
):
    nodes, columns, elements = value_ref.shape
    size = 8 * nodes
    rows = forward.shape[0] // 2
    radial = jnp.broadcast_to(radial_ref[...][:, None, :], (nodes, 8, elements)).reshape(
        size, elements
    )
    radial = jnp.concatenate([radial, radial], axis=1)
    shear = jnp.broadcast_to(shear_ref[...][:, None, :], (nodes, 8, elements))
    scale = jnp.broadcast_to((step_scale / mass_ref[...])[:, None, :], (nodes, 8, elements))

    def applied(matrix, x):
        high, low = split(x)
        both = dot(matrix[...], high)
        return both[:size] + both[rows : rows + size] + dot(matrix[0:rows, :], low)[:size]

    def body(index, carry):
        first = pl.multiple_of(index * 16 * CHAINS, 16 * CHAINS)
        starts = [first + 16 * chain for chain in range(CHAINS)]
        halves = [
            [value_ref[:, pl.ds(start, 8), :], value_ref[:, pl.ds(start + 8, 8), :]]
            for start in starts
        ]
        fields = [
            jnp.concatenate([half.reshape(size, elements) for half in pair], axis=1)
            for pair in halves
        ]
        fluxes = [radial * applied(forward, x) for x in fields]
        backs = [applied(backward, flux) for flux in fluxes]
        for start, pair, back in zip(starts, halves, backs):
            for side, half in enumerate(pair):
                part = pl.ds(start + 8 * side, 8)
                order = first_order + start + 8 * side + iota((8, elements), 0)
                wave = (2.0 * order.astype(f32) / MODES) ** 2
                block = back[:, side * elements : (side + 1) * elements]
                force = -block.reshape(nodes, 8, elements) - shear * wave[None] * half
                gain = jnp.where((order < modes_ref[...])[None], scale, 0.0)
                force_ref[:, part, :] = force
                drift_ref[:, part, :] = 2.0 * half - previous_ref[:, part, :] + gain * force
        return carry

    lax.fori_loop(0, columns // (16 * CHAINS), body, 0)


def transfers(pairs, done):
    return [
        pltpu.make_async_copy(source, target, done.at[index])
        for index, (source, target) in enumerate(pairs)
    ]


def begin(moves):
    for move in moves:
        move.start()


def finish(moves):
    for move in moves:
        move.wait()


def start_kernel(
    elements, box_ref, target_hbm, rows_hbm, lower_hbm, upper_hbm, derivative_hbm,
    value_hbm, radial_hbm, shear_hbm, mass_hbm, modes_hbm, previous_hbm,
    win_ref, off_hbm, cnt_hbm, picked_hbm, key_hbm, keycol_hbm, forward_hbm, backward_hbm, drift_hbm, low_hbm, high_hbm,
    target_ref, rows_ref, lower_ref, upper_ref, derivative_ref, value_ref, radial_ref, shear_ref,
    mass_ref, modes_ref, previous_ref,
    off_ref, cnt_ref, picked_ref, key_ref, keycol_ref, forward_ref, backward_ref, drift_ref, low_ref,
    high_ref, force_ref, stack_ref, done, kept,
):
    moves = transfers(
        [
            (target_hbm, target_ref), (rows_hbm, rows_ref), (lower_hbm, lower_ref),
            (upper_hbm, upper_ref), (derivative_hbm, derivative_ref), (value_hbm, value_ref),
            (radial_hbm, radial_ref), (shear_hbm, shear_ref), (mass_hbm, mass_ref),
            (modes_hbm, modes_ref), (previous_hbm, previous_ref),
        ],
        done,
    )
    saves = transfers(
        [
            (off_ref, off_hbm), (cnt_ref, cnt_hbm), (picked_ref, picked_hbm),
            (key_ref, key_hbm), (keycol_ref, keycol_hbm), (forward_ref, forward_hbm),
            (backward_ref, backward_hbm), (drift_ref, drift_hbm), (low_ref, low_hbm),
            (high_ref, high_hbm),
        ],
        kept,
    )
    begin(moves)
    finish(moves[:5])
    order_rows(
        elements, target_ref, rows_ref, lower_ref, upper_ref, key_ref, keycol_ref, off_ref,
        cnt_ref, win_ref,
    )
    columns = value_ref.shape[1]
    rows = forward_ref.shape[0] // 2
    forward_ref[...] = spread(derivative_ref, False, rows)
    backward_ref[...] = spread(derivative_ref, True, rows)
    begin(saves[:2] + saves[3:7])
    finish(moves[5:6])
    fill_stack(value_ref, stack_ref)
    pick_rows(stack_ref, key_ref, picked_ref)
    begin(saves[2:3])
    finish(moves[6:])
    force_into(
        value_ref, previous_ref, forward_ref, backward_ref, radial_ref, shear_ref, mass_ref,
        modes_ref, box_ref[0] * columns % MODES, force_ref, drift_ref,
    )
    begin(saves[7:8])
    fill_stack(force_ref, stack_ref)
    pick_boundary(stack_ref, key_ref, low_ref, high_ref, saves[8:])
    finish(saves)


def window_hot(win_ref, harmonic_ref, group, stride):
    window = pl.multiple_of(win_ref[0, group * stride], LANES)
    columns = harmonic_ref.shape[1] - 8
    place = harmonic_ref[group, columns : columns + 1, :].astype(i32)
    return window, hot(iota((WIDE, LANES), 0) + window == place)


def sample_into(win_ref, harmonic_ref, picked_ref, stride, sample_ref):
    columns = harmonic_ref.shape[1] - 8

    def body(index, carry):
        for group in [SAMPLES * index + part for part in range(SAMPLES)]:
            window, chosen = window_hot(win_ref, harmonic_ref, group, stride)
            rows = folded(dot(picked_ref[:, pl.ds(window, WIDE)], chosen))
            sample_ref[pl.ds(group, 1), :] = jnp.sum(
                rows * harmonic_ref[group, 0:columns, :], axis=0, keepdims=True
            )
        return carry

    lax.fori_loop(0, sample_ref.shape[0] // SAMPLES, body, 0)


def times(x, y):
    return x[0] * y[0] - x[1] * y[1], x[0] * y[1] + x[1] * y[0]


def node_kernel(
    stride, box_ref, win_ref, message_ref, off_hbm, cnt_hbm, picked_hbm,
    harmonic_ref, node_ref, sample_ref,
    off_ref, cnt_ref, picked_ref, place_ref, near_ref, far_re, far_im, done,
):
    moves = transfers(
        [(off_hbm, off_ref), (cnt_hbm, cnt_ref), (picked_hbm, picked_ref)], done
    )
    begin(moves)
    groups, columns = harmonic_ref.shape[0], harmonic_ref.shape[1] - 8
    place = message_ref[:, 0, :]
    angle = message_ref[:, 1, :]
    for index in range(5):
        node_ref[index] = message_ref[:, 2 + index, :]
    for bit in range(3):
        re, im = cos_sin(float(1 << bit) * angle)
        near_ref[2 * bit] = re
        near_ref[2 * bit + 1] = im
    first = box_ref[0] * columns
    base_re, base_im = cos_sin((first % MODES).astype(f32) * angle)
    sine = first >= MODES
    far = [
        (jnp.where(sine, base_im, base_re), jnp.where(sine, -base_re, base_im))
    ] + [None] * (columns // 8 - 1)
    bit = 1
    while bit < columns // 8:
        factor = cos_sin(float(8 * bit) * angle)
        for low in range(min(bit, columns // 8 - bit)):
            far[bit + low] = times(factor, far[low])
        bit *= 2
    for index, (re, im) in enumerate(far):
        far_re[index] = re
        far_im[index] = im
    finish(moves[:2])
    place_ref[...] = jnp.where(place < cnt_ref[...], off_ref[...] + place, -1.0)
    order = iota((8, LANES), 0)

    def body(index, carry):
        for group in [4 * index + part for part in range(4)]:
            row = pl.ds(group, 1)
            powers = [
                (
                    jnp.where((order >> bit) & 1 == 1, near_ref[2 * bit, row, :], 1.0),
                    jnp.where((order >> bit) & 1 == 1, near_ref[2 * bit + 1, row, :], 0.0),
                )
                for bit in range(3)
            ]
            re, im = times(times(powers[0], powers[1]), powers[2])
            for step in range(columns // 8):
                harmonic_ref[group, 8 * step : 8 * step + 8, :] = (
                    far_re[step, row, :] * re - far_im[step, row, :] * im
                )
            harmonic_ref[group, columns : columns + 8, :] = jnp.broadcast_to(
                place_ref[row, :], (8, LANES)
            )
        return carry

    lax.fori_loop(0, groups // 4, body, 0)
    finish(moves[2:])
    sample_into(win_ref, harmonic_ref, picked_ref, stride, sample_ref)


def nodes_step(samples_ref, node_ref, now, before, next_ref, coefficient_ref):
    sample = samples_ref[0]
    for index in range(1, samples_ref.shape[0]):
        sample = sample + samples_ref[index]
    pull = node_ref[0] * (sample - now)
    next_ref[...] = 2.0 * now - before + step_scale * pull / node_ref[1]
    coefficient_ref[...] = -node_ref[2] * pull


def react_into(win_ref, harmonic_ref, coefficient_ref, stride, reaction_ref):
    reaction_ref[...] = jnp.zeros_like(reaction_ref)
    columns = reaction_ref.shape[0]

    def react(index, carry):
        found = []
        for group in [BATCH * index + part for part in range(BATCH)]:
            window, chosen = window_hot(win_ref, harmonic_ref, group, stride)
            weighted = harmonic_ref[group, 0:columns, :] * coefficient_ref[pl.ds(group, 1), :]
            found.append((window, folded(dot_nt(stacked(weighted), chosen))))
        for window, rows in found:
            reaction_ref[:, pl.ds(window, WIDE)] = reaction_ref[:, pl.ds(window, WIDE)] + rows
        return carry

    lax.fori_loop(0, harmonic_ref.shape[0] // BATCH, react, 0)


def place_into(terms_ref, keycol_ref, elements, nodes, emit, flush):
    depth = terms_ref.shape[1]
    lane = iota((LANES, LANES), 1)

    def place_rows(first, width):
        sides = []
        for side in range(width):
            base = lane + (first + side) * elements
            chosen = [
                hot(keycol_ref[row : row + LANES, :] == base) for row in range(0, depth, LANES)
            ]
            sides.append(jnp.concatenate(chosen, axis=0))
        rows = folded(dot(terms_ref[...], jnp.concatenate(sides, axis=1)))
        for side in range(width):
            emit(first + side, rows[:, side * LANES : (side + 1) * LANES])

    def place_many(index, carry):
        for part in range(PAIRS):
            place_rows(2 * (PAIRS * index + part), 2)
        flush(2 * PAIRS * index, 2 * PAIRS, index)
        return carry

    steps = nodes // (2 * PAIRS)
    lax.fori_loop(0, steps, place_many, 0)
    for first in range(2 * PAIRS * steps, nodes, 2):
        place_rows(first, min(2, nodes - first))
    if nodes > 2 * PAIRS * steps:
        flush(2 * PAIRS * steps, nodes - 2 * PAIRS * steps, steps)


def annulus_step(
    early, late, after, flush, stride, first_order, win_ref, harmonic_ref, coefficient_ref,
    keycol_ref, below_ref, above_ref, drift_ref, mass_ref, modes_ref,
    next_ref, reaction_ref, terms_ref,
):
    nodes, columns, elements = drift_ref.shape
    count = reaction_ref.shape[1]
    shared = below_ref.shape[1]
    react_into(win_ref, harmonic_ref, coefficient_ref, stride, reaction_ref)
    finish(early)
    terms_ref[:, 0:count] = stacked(reaction_ref[...])
    terms_ref[:, count : count + shared] = stacked(below_ref[...])
    terms_ref[:, count + shared : count + 2 * shared] = stacked(above_ref[...])
    finish(late)
    live = first_order + iota((columns, elements), 0) < modes_ref[...]

    def emit(node, added):
        gain = jnp.where(live, step_scale / mass_ref[pl.ds(node, 1), :], 0.0)
        value = drift_ref[node] + gain * added
        next_ref[node] = value
        after(node, value)

    place_into(terms_ref, keycol_ref, elements, nodes, emit, flush)


def middle_kernel(
    stride, box_ref, win_ref, samples_ref, node_ref, harmonic_ref,
    keycol_hbm, below_hbm, above_hbm, drift_hbm, mass_hbm, modes_hbm,
    value_hbm, key_hbm, forward_hbm, backward_hbm, radial_hbm, shear_hbm,
    sample_ref, boxnext_ref, nextdrift_hbm, low_hbm, high_hbm,
    keycol_ref, below_ref, above_ref, drift_ref, mass_ref, modes_ref,
    value_ref, key_ref, forward_ref, backward_ref, radial_ref, shear_ref,
    next_ref, low_ref, high_ref,
    coefficient_ref, reaction_ref, terms_ref, force_ref, stack_ref, picked_ref,
    done, kept,
):
    moves = transfers(
        [
            (keycol_hbm, keycol_ref), (below_hbm, below_ref), (above_hbm, above_ref),
            (drift_hbm, drift_ref), (mass_hbm, mass_ref), (modes_hbm, modes_ref),
            (value_hbm, value_ref), (key_hbm, key_ref),
            (forward_hbm, forward_ref), (backward_hbm, backward_ref), (radial_hbm, radial_ref),
            (shear_hbm, shear_ref),
        ],
        done,
    )
    saves = transfers(
        [
            (drift_ref, nextdrift_hbm), (low_ref, low_hbm), (high_ref, high_hbm),
        ],
        kept,
    )
    begin(moves)
    columns = value_ref.shape[1]
    first_order = box_ref[0] * columns % MODES
    nodes_step(samples_ref, node_ref, node_ref[3], node_ref[4], boxnext_ref, coefficient_ref)
    elements = value_ref.shape[2]
    if stack_ref.shape[1] > value_ref.shape[0] * elements:
        tail = slice(value_ref.shape[0] * elements, stack_ref.shape[1])
        stack_ref[:, tail] = jnp.zeros_like(stack_ref[:, tail])

    def after(node, value):
        lanes = pl.ds(pl.multiple_of(node * elements, elements), elements)
        high, low = split(value)
        stack_ref[0:columns, lanes] = high
        stack_ref[columns:, lanes] = low

    annulus_step(
        moves[:3], moves[3:6], after, lambda first, size, index: None,
        stride, first_order, win_ref, harmonic_ref, coefficient_ref, keycol_ref,
        below_ref, above_ref, drift_ref, mass_ref, modes_ref,
        next_ref, reaction_ref, terms_ref,
    )
    finish(moves[6:])
    pick_rows(stack_ref, key_ref, picked_ref)
    force_into(
        next_ref, value_ref, forward_ref, backward_ref, radial_ref, shear_ref, mass_ref,
        modes_ref, first_order, force_ref, drift_ref,
    )
    begin(saves[:1])
    fill_stack(force_ref, stack_ref)
    pick_boundary(stack_ref, key_ref, low_ref, high_ref, saves[1:])
    sample_into(win_ref, harmonic_ref, picked_ref, stride, sample_ref)
    finish(saves)


def box_kernel(copies, box_ref, samples_ref, node_ref, now_ref, own_ref, coefficient_ref, *scratch):
    boxnext_ref = scratch[0] if scratch else own_ref
    nodes_step(samples_ref, node_ref, now_ref[...], node_ref[3], boxnext_ref, coefficient_ref)
    if scratch:
        for index in range(own_ref.shape[0]):
            own_ref[index : index + 1, :] = boxnext_ref[pl.ds(index * copies + box_ref[0], 1), :]


def last_kernel(
    stride, box_ref, win_ref, coefficient_ref, harmonic_ref,
    keycol_hbm, below_hbm, above_hbm, drift_hbm, mass_hbm, modes_hbm,
    next_hbm,
    keycol_ref, below_ref, above_ref, drift_ref, mass_ref, modes_ref,
    next_ref, reaction_ref, terms_ref, done, kept,
):
    moves = transfers(
        [
            (keycol_hbm, keycol_ref), (below_hbm, below_ref), (above_hbm, above_ref),
            (drift_hbm, drift_ref), (mass_hbm, mass_ref), (modes_hbm, modes_ref),
        ],
        done,
    )
    begin(moves)
    first_order = box_ref[0] * drift_ref.shape[1] % MODES

    def save(first, size, index):
        part = pl.ds(first, size)
        return pltpu.make_async_copy(next_ref.at[part], next_hbm.at[part], kept.at[index])

    annulus_step(
        moves[:3], moves[3:], lambda node, value: None,
        lambda first, size, index: save(first, size, index).start(),
        stride, first_order, win_ref, harmonic_ref, coefficient_ref, keycol_ref,
        below_ref, above_ref, drift_ref, mass_ref, modes_ref,
        next_ref, reaction_ref, terms_ref,
    )
    nodes = drift_ref.shape[0]
    steps = -(-nodes // (2 * PAIRS))
    finish(
        [
            save(2 * PAIRS * index, min(2 * PAIRS, nodes - 2 * PAIRS * index), index)
            for index in range(steps)
        ]
    )


def exchanged(low, high):
    size = lax.axis_size("mer")
    up = [(i, i + 1) for i in range(size - 1)]
    down = [(j, i) for i, j in up]
    return lax.ppermute(high, "mer", up), lax.ppermute(low, "mer", down)


SMEM, VMEM, HBM = pltpu.SMEM, pltpu.VMEM, pltpu.HBM


def call(kernel, ins, outs, scratch=(), copies=(), name=None, limit=40, flops=0):
    arrays = [
        pltpu.with_memory_space_constraint(array, memory) if pinned else array
        for array, memory, pinned in ins
    ]
    return pl.pallas_call(
        kernel,
        out_shape=[
            memory(shape, dtype) if memory else jax.ShapeDtypeStruct(shape, dtype)
            for shape, dtype, memory in outs
        ],
        in_specs=[pl.BlockSpec(memory_space=memory) for _, memory, _ in ins],
        out_specs=[pl.BlockSpec(memory_space=memory or VMEM) for _, _, memory in outs],
        scratch_shapes=[VMEM(shape, dtype) for shape, dtype in scratch]
        + [pltpu.SemaphoreType.DMA((number,)) for number in copies],
        compiler_params=pltpu.CompilerParams(vmem_limit_bytes=limit << 20),
        cost_estimate=pl.CostEstimate(flops=flops, transcendentals=0, bytes_accessed=0)
        if flops
        else None,
        name=name,
    )(*arrays)


def per_device(
    annulus,
    annulus_prev,
    derivative,
    radial_modulus,
    shear_modulus,
    node_mass,
    element_modes,
    upper_rows,
    lower_rows,
    coupling_rows,
    coupling_target,
    box_field,
    box_prev,
    box_angle,
    box_spring,
    box_mass,
    box_weight,
    box_slot,
):
    mer_count = lax.axis_size("mer")
    box_count = lax.axis_size("box")
    blocks = mer_count * box_count
    nodes, columns, elements = annulus.shape
    box_nodes = box_slot.shape[0]
    per = box_nodes // mer_count
    stride = LANES // per
    groups = blocks * per // LANES
    count = coupling_rows.shape[0]
    shared = upper_rows.shape[0]
    depth = count + 2 * shared
    padded_nodes = nodes + nodes % 2
    rows = -(-8 * nodes // 16) * 16
    volume = (nodes, columns, elements)
    grid = (groups, LANES)
    flat = (nodes, elements)
    stack_scratch = ((2 * columns, padded_nodes * elements), bf16)

    def far(value):
        return value, HBM, True

    def near(value):
        return value, VMEM, True

    def landed(value):
        return value, VMEM, False

    def anywhere(value):
        return value, pl.ANY, False

    def scalar(value):
        return value, SMEM, False

    box = scalar(jnp.full((1,), lax.axis_index("box"), i32))

    sent = [
        far(value.reshape(1, box_nodes))
        for value in (box_slot, box_angle, box_spring, box_mass, box_weight, box_field, box_prev)
    ]
    line = ((1, box_nodes), i32)
    messages, part, rank = call(
        functools.partial(group_kernel, mer_count, box_count),
        sent,
        [((blocks, 8, per), f32, VMEM), line + (HBM,), line + (HBM,)],
        [line, line, line, ((8, box_nodes), f32)],
        copies=(9,),
        name="group",
    )
    messages = lax.all_to_all(messages, ("mer", "box"), split_axis=0, concat_axis=0, tiled=True)
    if stride > 1:
        messages = messages.reshape(groups, stride, 8, per).swapaxes(1, 2)
        messages = messages.reshape(groups, 8, LANES)

    field = (volume, f32)
    table = (flat, f32)
    limits = ((1, elements), i32)
    modes = element_modes.reshape(1, elements)
    side = ((columns, shared), f32)
    keys = [((1, depth), i32), ((depth, LANES), i32)]
    matrices = [((2 * rows, 8 * nodes), bf16)] * 2
    picked = ((2 * columns, count), bf16)
    counts = ((blocks, LANES), f32)
    kept = [counts, counts, picked] + keys + matrices + [field, side, side]
    (
        window, offset, filled, chosen, key, keycol, forward, backward, drift, low, high,
    ) = call(
        functools.partial(start_kernel, elements),
        [
            box,
            far(coupling_target.reshape(1, count)),
            far(coupling_rows.reshape(1, count)),
            far(lower_rows.reshape(1, shared)),
            far(upper_rows.reshape(1, shared)),
            far(derivative),
            far(annulus),
            far(radial_modulus),
            far(shear_modulus),
            far(node_mass),
            far(modes),
            far(annulus_prev),
        ],
        [
            ((1, blocks), i32, None),
        ]
        + [shape + (HBM,) for shape in kept],
        [((1, count), i32)] * 2
        + [((1, shared), i32)] * 2
        + [((nodes, nodes), f32), field, table, table, table, limits, field]
        + kept
        + [field, stack_scratch],
        copies=(11, 10),
        name="start",
        flops=4 * columns * nodes * elements * (count + 2 * shared),
    )
    if stride > 1:
        offset = jnp.repeat(offset[:, 0], per).reshape(groups, LANES)
        filled = jnp.repeat(filled[:, 0], per).reshape(groups, LANES)
    window = scalar(window)
    below, above = exchanged(low, high)

    harmonic, node, sample = call(
        functools.partial(node_kernel, stride),
        [box, window, landed(messages), far(offset), far(filled), far(chosen)],
        [
            ((groups, columns + 8, LANES), f32, VMEM),
            ((5, groups, LANES), f32, VMEM),
            (grid, f32, None),
        ],
        [(grid, f32), (grid, f32), picked, (grid, f32)]
        + [((6, groups, LANES), f32)]
        + [((columns // 8, groups, LANES), f32)] * 2,
        copies=(3,),
        name="nodes",
        flops=4 * columns * groups * LANES * WIDE,
    )
    samples = lax.all_gather(sample, "box")

    fetched = keys[1:] + [side, side, field, table, limits]
    step_scratch = [
        ((columns, count), f32),
        ((2 * columns, depth), bf16),
    ]
    sample, box_now, drift, low, high = call(
        functools.partial(middle_kernel, stride),
        [
            box, window, landed(samples), near(node), near(harmonic),
            far(keycol), anywhere(below), anywhere(above), far(drift), far(node_mass), far(modes),
            far(annulus), far(key), far(forward), far(backward), far(radial_modulus),
            far(shear_modulus),
        ],
        [(grid, f32, None), (grid, f32, VMEM)]
        + [shape + (HBM,) for shape in (field, side, side)],
        fetched
        + [field]
        + keys[:1]
        + matrices
        + [table, table, field, side, side]
        + [(grid, f32)]
        + step_scratch
        + [field, stack_scratch, picked],
        copies=(12, 3),
        name="middle",
        flops=8 * columns * nodes * elements * (count + 2 * shared),
    )
    below, above = exchanged(low, high)
    samples = lax.all_gather(sample, "box")

    direct = stride == 1
    returned, coefficient = call(
        functools.partial(box_kernel, box_count),
        [box, landed(samples), near(node), near(box_now)],
        [((mer_count, per) if direct else grid, f32, VMEM), (grid, f32, VMEM)],
        [(grid, f32)] * direct,
        name="box",
    )
    if not direct:
        returned = lax.dynamic_index_in_dim(
            returned.reshape(mer_count, box_count, per), lax.axis_index("box"), axis=1, keepdims=False
        )
    returned = lax.all_to_all(returned, "mer", split_axis=0, concat_axis=0, tiled=True)
    (current,) = call(
        functools.partial(last_kernel, stride),
        [
            box, window, near(coefficient), near(harmonic), far(keycol), anywhere(below),
            anywhere(above), far(drift), far(node_mass), far(modes),
        ],
        [field + (HBM,)],
        fetched + [field] + step_scratch,
        copies=(6, -(-nodes // (2 * PAIRS))),
        name="last",
        flops=4 * columns * nodes * elements * (count + 2 * shared),
    )
    current, returned = lax.optimization_barrier((current, returned))
    (box_out,) = call(
        ungroup_kernel,
        [landed(part), landed(rank), landed(returned)],
        [((1, box_nodes), f32, None)],
        name="ungroup",
    )
    return current, box_out.reshape(box_nodes)


def solution(mesh):
    in_specs = (
        P(None, "box", "mer"),
        P(None, "box", "mer"),
        P(),
        P(None, "mer"),
        P(None, "mer"),
        P(None, "mer"),
        P("mer"),
        P("mer"),
        P("mer"),
        P("mer"),
        P("mer", None),
        P(("mer", "box")),
        P(("mer", "box")),
        P(("mer", "box")),
        P(("mer", "box")),
        P(("mer", "box")),
        P(("mer", "box")),
        P(("mer", "box")),
    )
    out_specs = (P(None, "box", "mer"), P(("mer", "box")))
    return jax.shard_map(
        per_device, mesh=mesh, in_specs=in_specs, out_specs=out_specs, check_vma=False
    )
```
